16 devices in a mesh: dp: 4 (over z, y), ep: 4 (over x, core).
Axes of the slice: x: 2, y: 2, z: 2, core: 2. Of those that a mesh axis runs over, the one named last changes fastest.
Arguments:
- hidden: bfloat16 [32768, 2304], P(('dp', 'ep')), parts along dimension 0
- ln_gamma: float32 [2304], replicated
- ln_beta: float32 [2304], replicated
- w_router: bfloat16 [2304, 8], replicated
- w_gate: bfloat16 [8, 2304, 5760], P('ep')
- w_up: bfloat16 [8, 2304, 5760], P('ep')
- w_down: bfloat16 [8, 5760, 2304], P('ep')
- choice: int32 [32768, 2], P(('dp', 'ep')), parts along dimension 0
- mask_first: int32 [32768, 8], P(('dp', 'ep')), parts along dimension 0
- mask_second: int32 [32768, 8], P(('dp', 'ep')), parts along dimension 0
Outputs:
- output: bfloat16 [32768, 2304], P(('dp', 'ep')), parts along dimension 0
There are 4 independent parts. The reference program is written for one: setup_inputs(seed, part) draws one part's arguments, and reference() takes and returns one part's arrays. A program takes and returns all parts, laid end to end along the dimension named above; an argument that names none is the same for every part.
All inputs are finite; a program needn't handle non-finite values.
Results may differ from the reference program's by a relative error of at most 0.001.
Values are sent between devices in bfloat16 or wider.
A program may use at most 1 GiB of HBM per device.

```python
import jax
import jax.numpy as jnp
from jax import lax

D_MODEL = 2304
FF_WIDTH = 5760
EXPERTS = 8
TOKENS_DEV = 2048
GROUP_DEVS = 4
TOKENS = GROUP_DEVS * TOKENS_DEV
CAPACITY = (10 * TOKENS_DEV + 4 * EXPERTS - 1) // (4 * EXPERTS)
LN_EPS = 1e-5


def draw_routing(route_key):
    sub_keys = jax.random.split(route_key, 6)
    favoured = jax.random.randint(sub_keys[0], (), 0, EXPERTS)
    coin_flip = jax.random.randint(sub_keys[1], (TOKENS,), 0, 4)
    spread = jax.random.randint(sub_keys[2], (TOKENS,), 0, EXPERTS)
    first_pick = jnp.where(coin_flip == 0, favoured, spread)
    second_pick = (first_pick + 1 + jax.random.randint(sub_keys[3], (TOKENS,), 0, EXPERTS - 1)) % EXPERTS
    expert_ids = jnp.arange(EXPERTS)
    is_first = first_pick[:, None] == expert_ids
    is_second = second_pick[:, None] == expert_ids
    keep_first = jax.random.randint(sub_keys[4], (TOKENS, EXPERTS), 0, 4) == 0
    keep_second = jax.random.randint(sub_keys[5], (TOKENS, EXPERTS), 0, 4) == 0
    mask_first = (keep_first | is_first).astype(jnp.int32)
    mask_second = ((keep_second | is_second) & (~is_first)).astype(jnp.int32)
    choice = jnp.stack([first_pick, second_pick], axis=1).astype(jnp.int32)
    return choice, mask_first, mask_second


def setup_inputs(seed: int = 0, part: int = 0) -> dict:
    shared_keys = jax.random.split(jax.random.key(seed), 6)
    part_keys = jax.random.split(jax.random.fold_in(jax.random.key(seed + 1), part), 2)
    hidden = jax.random.normal(part_keys[0], (TOKENS, D_MODEL), jnp.float32).astype(jnp.bfloat16)
    choice, mask_first, mask_second = draw_routing(part_keys[1])
    ln_gamma = 1.0 + 0.4 * jax.random.normal(shared_keys[0], (D_MODEL,), jnp.float32)
    ln_beta = 0.4 * jax.random.normal(shared_keys[1], (D_MODEL,), jnp.float32)
    w_router = (jax.random.normal(shared_keys[2], (D_MODEL, EXPERTS), jnp.float32) * D_MODEL ** -0.5).astype(jnp.bfloat16)
    w_gate = (jax.random.normal(shared_keys[3], (EXPERTS, D_MODEL, FF_WIDTH), jnp.float32) * D_MODEL ** -0.5).astype(jnp.bfloat16)
    w_up = (jax.random.normal(shared_keys[4], (EXPERTS, D_MODEL, FF_WIDTH), jnp.float32) * D_MODEL ** -0.5).astype(jnp.bfloat16)
    w_down = (jax.random.normal(shared_keys[5], (EXPERTS, FF_WIDTH, D_MODEL), jnp.float32) * FF_WIDTH ** -0.5).astype(jnp.bfloat16)
    return {"hidden": hidden, "ln_gamma": ln_gamma, "ln_beta": ln_beta, "w_router": w_router,
            "w_gate": w_gate, "w_up": w_up, "w_down": w_down, "choice": choice,
            "mask_first": mask_first, "mask_second": mask_second}


def layer_norm(token_rows, ln_gamma, ln_beta):
    values = token_rows.astype(jnp.float32)
    centred = values - jnp.mean(values, axis=-1, keepdims=True)
    variance = jnp.mean(centred * centred, axis=-1, keepdims=True)
    return (centred * lax.rsqrt(variance + LN_EPS) * ln_gamma + ln_beta).astype(jnp.bfloat16)


def reference(hidden, ln_gamma, ln_beta, w_router, w_gate, w_up, w_down, choice, mask_first, mask_second):
    normed = layer_norm(hidden, ln_gamma, ln_beta)
    scores = jnp.dot(normed, w_router, preferred_element_type=jnp.float32)
    mask_pair = jnp.stack([mask_first, mask_second], axis=1) > 0
    soft_probs = jax.nn.softmax(jnp.where(mask_pair, scores[:, None, :], -jnp.inf), axis=-1)
    gate_vals = jnp.take_along_axis(soft_probs, choice[:, :, None], axis=-1)[:, :, 0]
    by_source = choice.reshape(GROUP_DEVS, TOKENS_DEV, 2)
    expert_ids = jnp.arange(EXPERTS, dtype=jnp.int32)
    hit_count = (by_source[..., None] == expert_ids).astype(jnp.int32)
    per_token = jnp.sum(hit_count, axis=2)
    before = jnp.cumsum(per_token, axis=1) - per_token
    position = jnp.take_along_axis(before, by_source, axis=2)
    kept_copy = position < CAPACITY
    source_ids = jnp.broadcast_to(jnp.arange(GROUP_DEVS, dtype=jnp.int32)[:, None, None], by_source.shape)
    token_ids = jnp.broadcast_to(jnp.arange(TOKENS, dtype=jnp.int32).reshape(GROUP_DEVS, TOKENS_DEV, 1), by_source.shape)
    slot_table = jnp.zeros((EXPERTS, GROUP_DEVS, CAPACITY), jnp.int32)
    slot_table = slot_table.at[by_source, source_ids, position].set(token_ids, mode="drop")

    def one_expert(operands):
        row_index, gate_mat, up_mat, down_mat = operands
        expert_rows = normed[row_index.reshape(-1)]
        gate_proj = jnp.dot(expert_rows, gate_mat, preferred_element_type=jnp.float32)
        up_proj = jnp.dot(expert_rows, up_mat, preferred_element_type=jnp.float32)
        inner_act = (jax.nn.silu(gate_proj) * up_proj).astype(jnp.bfloat16)
        return jnp.dot(inner_act, down_mat, preferred_element_type=jnp.float32).astype(jnp.bfloat16)

    expert_out = lax.map(one_expert, (slot_table, w_gate, w_up, w_down))
    expert_out = expert_out.reshape(EXPERTS, GROUP_DEVS, CAPACITY, D_MODEL)
    picked = expert_out[by_source, source_ids, jnp.minimum(position, CAPACITY - 1)]
    kept_gates = jnp.where(kept_copy, gate_vals.reshape(GROUP_DEVS, TOKENS_DEV, 2), 0.0)
    mixed_out = hidden.reshape(GROUP_DEVS, TOKENS_DEV, D_MODEL).astype(jnp.float32) + jnp.sum(kept_gates[..., None] * picked.astype(jnp.float32), axis=2)
    return mixed_out.reshape(TOKENS, D_MODEL).astype(jnp.bfloat16)
```

```python
import functools

import jax
import jax.numpy as jnp
from jax import lax
from jax.experimental import pallas as pl
from jax.experimental.pallas import tpu as pltpu
from jax.sharding import PartitionSpec as P


LN_EPS = 1e-5
F32, BF16, I32 = jnp.float32, jnp.bfloat16, jnp.int32
VMEM_LIMIT = 66 * 1024 * 1024 - 2 * 1024 * 1024 - 128 * 1024
NORM_ROWS = 256
PACK_ROWS = 256
PACK_WIN = 128
TILE = 160
FF_BLOCK = 768
MIX_ROWS = 128
MIX_WIN = 256


def norm_kernel(x_ref, gamma_ref, beta_ref, router_ref, choice_ref, rel_ref, first_ref, second_ref, u_ref, gate_ref):
    values = x_ref[...].astype(F32)
    centred = values - jnp.mean(values, axis=-1, keepdims=True)
    variance = jnp.mean(centred * centred, axis=-1, keepdims=True)
    normed = (centred * lax.rsqrt(variance + LN_EPS) * gamma_ref[...] + beta_ref[...]).astype(BF16)
    u_ref[...] = normed
    scores = lax.dot_general(router_ref[...], normed, (((1,), (1,)), ((), ())), preferred_element_type=F32)
    expert_ids = lax.broadcasted_iota(I32, scores.shape, 0)
    gates = jnp.zeros_like(scores)
    for j, mask_ref in enumerate((first_ref, second_ref)):
        masked = jnp.where(mask_ref[...] > 0, scores, -jnp.inf)
        weights = jnp.exp(masked - jnp.max(masked, axis=0, keepdims=True))
        picked = jnp.where(expert_ids == choice_ref[j:j + 1, :], weights, 0.0)
        gate = jnp.sum(picked, axis=0, keepdims=True) / jnp.sum(weights, axis=0, keepdims=True)
        gates = gates + jnp.where(expert_ids == rel_ref[j:j + 1, :], gate, 0.0)
    gate_ref[...] = gates


def norm_call(part, parts, hidden, gamma, beta, router_t, choice_t, rel_t, first_t, second_t):
    tokens, width = hidden.shape
    experts = router_t.shape[0]
    rows = tokens // parts
    steps = rows // NORM_ROWS
    at = lambda i: i + part * steps
    lanes = lambda n: pl.BlockSpec((n, NORM_ROWS), lambda i: (0, at(i)))
    whole = lambda shape: pl.BlockSpec(shape, lambda i: (0, 0))
    return pl.pallas_call(
        norm_kernel,
        grid=(steps,),
        in_specs=[pl.BlockSpec((NORM_ROWS, width), lambda i: (at(i), 0)), whole((1, width)), whole((1, width)),
                  whole((experts, width)), lanes(2), lanes(2), lanes(experts), lanes(experts)],
        out_specs=[pl.BlockSpec((NORM_ROWS, width), lambda i: (i, 0)),
                   pl.BlockSpec((experts, NORM_ROWS), lambda i: (0, i))],
        out_shape=[jax.ShapeDtypeStruct((rows, width), BF16), jax.ShapeDtypeStruct((experts, rows), F32)],
        cost_estimate=pl.CostEstimate(flops=rows * width * 60, bytes_accessed=rows * width * 4, transcendentals=0),
        name="norm",
    )(hidden, gamma, beta, router_t, choice_t, rel_t, first_t, second_t)


def pack_kernel(half_steps, start_ref, pos_ref, low_ref, high_ref, rows_ref):
    step = pl.program_id(0)
    experts = rows_ref.shape[0]
    steps = 2 * half_steps

    @pl.when(step == 0)
    def _():
        rows_ref[...] = jnp.zeros_like(rows_ref)

    def pack(block_ref):
        for e in range(experts):
            begin = start_ref[e * (steps + 1) + step]
            end = start_ref[e * (steps + 1) + step + 1]
            base = (begin // 16) * 16
            windows = jnp.where(end > begin, (end - base + PACK_WIN - 1) // PACK_WIN, 0)
            slots = jnp.broadcast_to(pos_ref[e:e + 1, :], (PACK_WIN, PACK_ROWS))
            sublane = lax.broadcasted_iota(I32, (PACK_WIN, PACK_ROWS), 0)

            def window(w, carry):
                at = pl.multiple_of(base + w * PACK_WIN, 16)
                onehot = (slots - at == sublane).astype(F32).astype(BF16)
                picked = jnp.dot(onehot, block_ref[...], preferred_element_type=F32)
                held = rows_ref[e, pl.ds(at, PACK_WIN), :]
                rows_ref[e, pl.ds(at, PACK_WIN), :] = (held.astype(F32) + picked).astype(BF16)
                return carry

            lax.fori_loop(0, windows, window, 0)

    pl.when(step < half_steps)(lambda: pack(low_ref))
    pl.when(step >= half_steps)(lambda: pack(high_ref))


def pack_call(starts, pos, low, high, capacity):
    half, width = low.shape
    experts = pos.shape[0]
    half_steps = half // PACK_ROWS
    padded = (capacity + PACK_WIN - 1) // PACK_WIN * PACK_WIN + PACK_WIN
    return pl.pallas_call(
        functools.partial(pack_kernel, half_steps),
        grid_spec=pltpu.PrefetchScalarGridSpec(
            num_scalar_prefetch=1,
            grid=(2 * half_steps,),
            in_specs=[pl.BlockSpec((experts, PACK_ROWS), lambda i, s: (0, i)),
                      pl.BlockSpec((PACK_ROWS, width), lambda i, s: (jnp.minimum(i, half_steps - 1), 0)),
                      pl.BlockSpec((PACK_ROWS, width), lambda i, s: (jnp.maximum(i - half_steps, 0), 0))],
            out_specs=pl.BlockSpec((experts, padded, width), lambda i, s: (0, 0, 0)),
        ),
        out_shape=jax.ShapeDtypeStruct((experts, padded, width), BF16),
        compiler_params=pltpu.CompilerParams(vmem_limit_bytes=40 * 1024 * 1024),
        cost_estimate=pl.CostEstimate(flops=experts * 2 * half * PACK_ROWS * width, bytes_accessed=4 * half * width * 3,
                                      transcendentals=0),
        name="pack",
    )(starts, pos, low, high)


def mlp_kernel(full_steps, tail, tiles_ref, one_ref, two_ref, gate_ref, up_ref, down_ref, out_one_ref, out_two_ref, acc_ref):
    step = pl.program_id(0)
    tiles = tiles_ref[0]
    rows = out_one_ref.shape[0]

    @pl.when(step == 0)
    def _():
        acc_ref[...] = jnp.zeros_like(acc_ref)

    def accumulate(width):
        def tile(i, carry):
            at = pl.multiple_of(i * TILE, TILE)
            both = pl.multiple_of(i * 2 * TILE, 2 * TILE)
            tokens = jnp.concatenate([one_ref[0, pl.ds(at, TILE), :], two_ref[0, pl.ds(at, TILE), :]], axis=0)
            joined = jnp.concatenate([gate_ref[0, :, :width], up_ref[0, :, :width]], axis=1)
            proj = jnp.dot(tokens, joined, preferred_element_type=F32)
            inner = (jax.nn.silu(proj[:, :width]) * proj[:, width:]).astype(BF16)
            acc_ref[pl.ds(both, 2 * TILE), :] += jnp.dot(inner, down_ref[0, :width, :], preferred_element_type=F32)
            return carry

        lax.fori_loop(0, tiles, tile, 0)

    pl.when(step < full_steps)(lambda: accumulate(FF_BLOCK))

    @pl.when(step == full_steps)
    def _():
        accumulate(tail)
        for i in range(rows // TILE):
            out_one_ref[i * TILE:(i + 1) * TILE, :] = acc_ref[2 * i * TILE:(2 * i + 1) * TILE, :].astype(BF16)
            out_two_ref[i * TILE:(i + 1) * TILE, :] = acc_ref[(2 * i + 1) * TILE:(2 * i + 2) * TILE, :].astype(BF16)


def mlp_call(expert, chunk, rows, tiles, packed_one, packed_two, w_gate, w_up, w_down):
    width, ff = w_gate.shape[1:]
    full_steps, tail = divmod(ff, FF_BLOCK)
    once = pl.Buffered(1)
    packed_spec = pl.BlockSpec((1, rows, width), lambda f, t: (expert, chunk, 0), pipeline_mode=once)
    out_spec = pl.BlockSpec((rows, width), lambda f, t: (0, 0), pipeline_mode=once)
    in_spec = pl.BlockSpec((1, width, FF_BLOCK), lambda f, t: (expert, 0, f))
    out = jax.ShapeDtypeStruct((rows, width), BF16)
    return pl.pallas_call(
        functools.partial(mlp_kernel, full_steps, tail),
        grid_spec=pltpu.PrefetchScalarGridSpec(
            num_scalar_prefetch=1,
            grid=(full_steps + 1,),
            in_specs=[packed_spec, packed_spec, in_spec, in_spec,
                      pl.BlockSpec((1, FF_BLOCK, width), lambda f, t: (expert, f, 0))],
            out_specs=[out_spec, out_spec],
            scratch_shapes=[pltpu.VMEM((2 * rows, width), F32)],
        ),
        out_shape=[out, out],
        compiler_params=pltpu.CompilerParams(vmem_limit_bytes=VMEM_LIMIT),
        cost_estimate=pl.CostEstimate(flops=6 * 2 * rows * width * ff, bytes_accessed=6 * width * ff, transcendentals=0),
        name="mlp",
    )(tiles, packed_one, packed_two, w_gate, w_up, w_down)


def mix_kernel(columns, pieces, capacity, start_ref, base_ref, pos_ref, gate_ref, *rest):
    piece_refs, (out_ref, held_ref, sem) = rest[:-3], rest[-3:]
    step = pl.program_id(0)
    steps = pl.num_programs(0)

    @pl.when(step == 0)
    def _():
        copies = []
        for n, piece in enumerate(piece_refs):
            rows = piece.shape[0]
            copies.append(pltpu.make_async_copy(
                piece, held_ref.at[n // pieces, pl.ds((n % pieces) * rows, rows), :], sem.at[n]))
        for copy in copies:
            copy.start()
        for copy in copies:
            copy.wait()

    total = base_ref[...].astype(F32)
    lane = lax.broadcasted_iota(I32, (MIX_ROWS, MIX_WIN), 1)
    for n, column in enumerate(columns):
        begin = start_ref[column * (steps + 1) + step]
        base = pl.multiple_of(jnp.minimum((begin // 16) * 16, capacity - MIX_WIN), 16)
        onehot = (pos_ref[:, column:column + 1] - base == lane).astype(F32).astype(BF16)
        picked = jnp.dot(onehot, held_ref[n, pl.ds(base, MIX_WIN), :], preferred_element_type=F32)
        total = total + gate_ref[:, column:column + 1] * picked
    out_ref[...] = total.astype(out_ref.dtype)


def mix_call(columns, pieces, capacity, starts, base, pos, gates, rows, out_dtype):
    tokens, width = base.shape
    block = pl.BlockSpec((MIX_ROWS, width), lambda i, s: (i, 0))
    small = pl.BlockSpec((MIX_ROWS, pos.shape[1]), lambda i, s: (i, 0))
    return pl.pallas_call(
        functools.partial(mix_kernel, columns, pieces, capacity),
        grid_spec=pltpu.PrefetchScalarGridSpec(
            num_scalar_prefetch=1,
            grid=(tokens // MIX_ROWS,),
            in_specs=[block, small, small] + [pl.BlockSpec(memory_space=pl.ANY)] * len(rows),
            out_specs=block,
            scratch_shapes=[pltpu.VMEM((len(columns), capacity, width), BF16), pltpu.SemaphoreType.DMA((len(rows),))],
        ),
        out_shape=jax.ShapeDtypeStruct((tokens, width), out_dtype),
        compiler_params=pltpu.CompilerParams(vmem_limit_bytes=48 * 1024 * 1024),
        cost_estimate=pl.CostEstimate(flops=2 * tokens * MIX_WIN * width * len(columns),
                                      bytes_accessed=tokens * width * 10, transcendentals=0),
        name="mix",
    )(starts, base, pos, gates, *rows)


def solution(mesh):
    group_size = mesh.shape["ep"]
    rows_spec = P(("dp", "ep"))

    def swap(array, distance):
        return lax.ppermute(array, "ep", [(i, i ^ distance) for i in range(group_size)])

    def device_step(hidden, ln_gamma, ln_beta, w_router, w_gate, w_up, w_down, choice, mask_first, mask_second):
        tokens, _ = hidden.shape
        local = w_gate.shape[0]
        experts = local * group_size
        capacity = (10 * tokens + 4 * experts - 1) // (4 * experts)
        chunks = 2
        chunk_rows = capacity // chunks

        choice_t = choice.T
        rel_t = choice_t ^ (local * lax.axis_index("ep"))
        ids = lax.broadcasted_iota(I32, (experts, 1), 0)
        hit = ((rel_t[0:1] == ids) | (rel_t[1:2] == ids)).astype(I32)
        through = jnp.cumsum(hit, axis=1)
        before = through - hit
        pos = jnp.where((hit > 0) & (before < capacity), before, -1)
        starts = jnp.minimum(jnp.concatenate([before[:, ::MIX_ROWS], through[:, -1:]], axis=1), capacity)
        pack_starts = starts[:, ::PACK_ROWS // MIX_ROWS]
        marks = pack_starts.shape[1]
        meta = jnp.concatenate([pos, jnp.pad(pack_starts, ((0, 0), (0, 128 - marks)))], axis=1)
        metas = [meta[:local]] + [swap(meta[local * m:local * (m + 1)], m) for m in range(1, group_size)]

        halves, gates = [], []
        for part in range(2):
            u, g = norm_call(part, 2, hidden, ln_gamma[None], ln_beta[None], w_router.T, choice_t, rel_t,
                             mask_first.T, mask_second.T)
            halves.append(u)
            gates.append(g)
        gates_t = jnp.concatenate(gates, axis=1).T
        pos_t = pos.T

        sources = [halves, [swap(u, 1) for u in halves], [swap(u, 2) for u in halves]]
        sources.append([swap(u, 1) for u in sources[2]])

        def pack(m):
            return pack_call(metas[m][:, tokens:tokens + marks].reshape(-1), metas[m][:, :tokens], *sources[m], capacity)

        def counts(m):
            return metas[m][:, tokens + marks - 1]

        def run(m_one, m_two, expert, chunk, rows, packed):
            most = jnp.maximum(counts(m_one)[expert], counts(m_two)[expert])
            tiles = jnp.clip((most + TILE - 1) // TILE - chunk * (rows // TILE), 0, rows // TILE)
            return mlp_call(expert, chunk, rows, tiles[None], *packed, w_gate, w_up, w_down)

        near = [pack(0), pack(1)]
        near_rows = []
        for e in range(local):
            near_rows.append(run(0, 1, e, 0, capacity, near))
        mine = [one for one, _ in near_rows] + [swap(two, 1) for _, two in near_rows]

        far = [pack(2), pack(3)]
        far_two, far_three = [], []
        for e in range(local):
            for c in range(chunks):
                one, two = run(2, 3, e, c, chunk_rows, far)
                far_two.append(swap(one, 2))
                far_three.append(swap(two, 3))

        flat = starts.reshape(-1)
        total = mix_call(tuple(range(2 * local)), 1, capacity, flat, hidden, pos_t, gates_t, mine, F32)
        return mix_call(tuple(range(2 * local, experts)), chunks, capacity, flat, total, pos_t, gates_t,
                        far_two + far_three, BF16)

    return jax.shard_map(device_step, mesh=mesh,
                         in_specs=(rows_spec, P(), P(), P(), P("ep"), P("ep"), P("ep"), rows_spec, rows_spec, rows_spec),
                         out_specs=rows_spec, check_vma=False)
```

```python
import functools

import jax
import jax.numpy as jnp
from jax import lax
from jax.experimental import pallas as pl
from jax.experimental.pallas import tpu as pltpu
from jax.sharding import PartitionSpec as P


LN_EPS = 1e-5
F32, BF16, I32 = jnp.float32, jnp.bfloat16, jnp.int32
VMEM_LIMIT = 67043328
NORM_ROWS = 256
PACK_ROWS = 512
PACK_WIN = 128
TILE = 160
FF_BLOCK = 1280
FF_SPLIT = 768
MIX_ROWS = 128
MIX_WIN = 256
MIX_COLS = 256


def norm_kernel(x_ref, gamma_ref, beta_ref, u_ref):
    values = x_ref[...].astype(F32)
    centred = values - jnp.mean(values, axis=-1, keepdims=True)
    variance = jnp.mean(centred * centred, axis=-1, keepdims=True)
    u_ref[...] = (centred * lax.rsqrt(variance + LN_EPS) * gamma_ref[...] + beta_ref[...]).astype(BF16)


def norm_call(part, parts, hidden, gamma, beta):
    tokens, width = hidden.shape
    rows = tokens // parts
    steps = rows // NORM_ROWS
    vector = pl.BlockSpec((1, width), lambda i: (0, 0))
    return pl.pallas_call(
        norm_kernel,
        grid=(steps,),
        in_specs=[pl.BlockSpec((NORM_ROWS, width), lambda i: (i + part * steps, 0)), vector, vector],
        out_specs=pl.BlockSpec((NORM_ROWS, width), lambda i: (i, 0)),
        out_shape=jax.ShapeDtypeStruct((rows, width), BF16),
        compiler_params=pltpu.CompilerParams(vmem_limit_bytes=VMEM_LIMIT),
        cost_estimate=pl.CostEstimate(flops=rows * width * 60, bytes_accessed=rows * width * 4, transcendentals=0),
        name="norm",
    )(hidden, gamma, beta)


def gate_kernel(u_ref, router_ref, choice_ref, rel_ref, first_ref, second_ref, gate_ref):
    scores = lax.dot_general(router_ref[...], u_ref[...], (((1,), (1,)), ((), ())), preferred_element_type=F32)
    expert_ids = lax.broadcasted_iota(I32, scores.shape, 0)
    gates = jnp.zeros_like(scores)
    for j, mask_ref in enumerate((first_ref, second_ref)):
        masked = jnp.where(mask_ref[...] > 0, scores, -jnp.inf)
        weights = jnp.exp(masked - jnp.max(masked, axis=0, keepdims=True))
        picked = jnp.where(expert_ids == choice_ref[j:j + 1, :], weights, 0.0)
        gate = jnp.sum(picked, axis=0, keepdims=True) / jnp.sum(weights, axis=0, keepdims=True)
        gates = gates + jnp.where(expert_ids == rel_ref[j:j + 1, :], gate, 0.0)
    gate_ref[...] = gates


def gate_call(part, u, router_t, choice_t, rel_t, first_t, second_t):
    rows, width = u.shape
    experts = router_t.shape[0]
    steps = rows // NORM_ROWS
    lanes = lambda n: pl.BlockSpec((n, NORM_ROWS), lambda i: (0, i + part * steps))
    return pl.pallas_call(
        gate_kernel,
        grid=(steps,),
        in_specs=[pl.BlockSpec((NORM_ROWS, width), lambda i: (i, 0)), pl.BlockSpec((experts, width), lambda i: (0, 0)),
                  lanes(2), lanes(2), lanes(experts), lanes(experts)],
        out_specs=pl.BlockSpec((experts, NORM_ROWS), lambda i: (0, i)),
        out_shape=jax.ShapeDtypeStruct((experts, rows), F32),
        compiler_params=pltpu.CompilerParams(vmem_limit_bytes=VMEM_LIMIT),
        cost_estimate=pl.CostEstimate(flops=rows * width * 60, bytes_accessed=rows * width * 2, transcendentals=0),
        name="gate",
    )(u, router_t, choice_t, rel_t, first_t, second_t)


def pack_kernel(half_steps, start_ref, pos_ref, low_ref, high_ref, rows_ref):
    step = pl.program_id(0)
    experts = rows_ref.shape[0]
    steps = 2 * half_steps

    @pl.when(step == 0)
    def _():
        rows_ref[...] = jnp.zeros_like(rows_ref)

    def pack(block_ref):
        for e in range(experts):
            begin = start_ref[e * (steps + 1) + step]
            end = start_ref[e * (steps + 1) + step + 1]
            base = (begin // 16) * 16
            windows = jnp.where(end > begin, (end - base + PACK_WIN - 1) // PACK_WIN, 0)
            slots = jnp.broadcast_to(pos_ref[e:e + 1, :], (PACK_WIN, PACK_ROWS))
            sublane = lax.broadcasted_iota(I32, (PACK_WIN, PACK_ROWS), 0)

            def window(w, carry):
                at = pl.multiple_of(base + w * PACK_WIN, 16)
                onehot = (slots - at == sublane).astype(F32).astype(BF16)
                picked = jnp.dot(onehot, block_ref[...], preferred_element_type=F32)
                held = rows_ref[e, pl.ds(at, PACK_WIN), :]
                rows_ref[e, pl.ds(at, PACK_WIN), :] = (held.astype(F32) + picked).astype(BF16)
                return carry

            lax.fori_loop(0, windows, window, 0)

    pl.when(step < half_steps)(lambda: pack(low_ref))
    pl.when(step >= half_steps)(lambda: pack(high_ref))


def pack_call(starts, pos, low, high, capacity):
    half, width = low.shape
    experts = pos.shape[0]
    half_steps = half // PACK_ROWS
    padded = (capacity + PACK_WIN - 1) // PACK_WIN * PACK_WIN + PACK_WIN
    return pl.pallas_call(
        functools.partial(pack_kernel, half_steps),
        grid_spec=pltpu.PrefetchScalarGridSpec(
            num_scalar_prefetch=1,
            grid=(2 * half_steps,),
            in_specs=[pl.BlockSpec((experts, PACK_ROWS), lambda i, s: (0, i)),
                      pl.BlockSpec((PACK_ROWS, width), lambda i, s: (jnp.minimum(i, half_steps - 1), 0)),
                      pl.BlockSpec((PACK_ROWS, width), lambda i, s: (jnp.maximum(i - half_steps, 0), 0))],
            out_specs=pl.BlockSpec((experts, padded, width), lambda i, s: (0, 0, 0)),
        ),
        out_shape=jax.ShapeDtypeStruct((experts, padded, width), BF16),
        compiler_params=pltpu.CompilerParams(vmem_limit_bytes=VMEM_LIMIT),
        cost_estimate=pl.CostEstimate(flops=experts * 2 * half * PACK_ROWS * width, bytes_accessed=4 * half * width * 3,
                                      transcendentals=0),
        name="pack",
    )(starts, pos, low, high)


def mlp_kernel(splits, tail_splits, tiles_ref, one_ref, two_ref, gate_ref, up_ref, down_ref, out_one_ref, out_two_ref, acc_ref):
    step = pl.program_id(1)
    tiles = tiles_ref[pl.program_id(0)]
    rows = out_one_ref.shape[1]

    def accumulate(parts, first):
        def tile(i, carry):
            at = pl.multiple_of(i * TILE, TILE)
            both = pl.ds(pl.multiple_of(i * 2 * TILE, 2 * TILE), 2 * TILE)
            tokens = jnp.concatenate([one_ref[0, pl.ds(at, TILE), :], two_ref[0, pl.ds(at, TILE), :]], axis=0)
            projs = []
            for lo, hi in parts:
                joined = jnp.concatenate([gate_ref[0, :, lo:hi], up_ref[0, :, lo:hi]], axis=1)
                projs.append(jnp.dot(tokens, joined, preferred_element_type=F32))
            for n, (lo, hi) in enumerate(parts):
                inner = (jax.nn.silu(projs[n][:, :hi - lo]) * projs[n][:, hi - lo:]).astype(BF16)
                down = jnp.dot(inner, down_ref[0, lo:hi, :], preferred_element_type=F32)
                if first and n == 0:
                    acc_ref[both, :] = down
                else:
                    acc_ref[both, :] += down
            return carry

        lax.fori_loop(0, tiles, tile, 0)

    pl.when(step == 0)(lambda: accumulate(tail_splits, True))
    pl.when(step > 0)(lambda: accumulate(splits, False))

    @pl.when(step == pl.num_programs(1) - 1)
    def _():
        for i in range(rows // TILE):
            outs = [(ref, (2 * i + n) * TILE) for n, ref in enumerate((out_one_ref, out_two_ref))]

            @pl.when(i < tiles)
            def _():
                for ref, at in outs:
                    ref[0, i * TILE:(i + 1) * TILE, :] = acc_ref[at:at + TILE, :].astype(BF16)

            @pl.when(i >= tiles)
            def _():
                for ref, _at in outs:
                    ref[0, i * TILE:(i + 1) * TILE, :] = jnp.zeros((TILE, ref.shape[2]), BF16)


def mlp_call(rows, chunk, tiles, packed_one, packed_two, w_gate, w_up, w_down):
    experts, width, ff = w_gate.shape
    full_steps, tail = divmod(ff, FF_BLOCK)
    splits = ((0, FF_SPLIT), (FF_SPLIT, FF_BLOCK))
    tail_splits = ((0, tail),)
    once = pl.Buffered(1)

    def block(e, f, t):
        return jnp.where((f == 0) | (t[e] == 0), full_steps, f - 1)

    packed_spec = pl.BlockSpec((1, rows, width), lambda e, f, t: (e, chunk, 0), pipeline_mode=once)
    out_spec = pl.BlockSpec((1, rows, width), lambda e, f, t: (e, 0, 0), pipeline_mode=once)
    in_spec = pl.BlockSpec((1, width, FF_BLOCK), lambda e, f, t: (e, 0, block(e, f, t)))
    out = jax.ShapeDtypeStruct((experts, rows, width), BF16)
    return pl.pallas_call(
        functools.partial(mlp_kernel, splits, tail_splits),
        grid_spec=pltpu.PrefetchScalarGridSpec(
            num_scalar_prefetch=1,
            grid=(experts, full_steps + 1),
            in_specs=[packed_spec, packed_spec, in_spec, in_spec,
                      pl.BlockSpec((1, FF_BLOCK, width), lambda e, f, t: (e, block(e, f, t), 0))],
            out_specs=[out_spec, out_spec],
            scratch_shapes=[pltpu.VMEM((2 * rows, width), F32)],
        ),
        out_shape=[out, out],
        compiler_params=pltpu.CompilerParams(vmem_limit_bytes=VMEM_LIMIT),
        cost_estimate=pl.CostEstimate(flops=6 * 2 * experts * rows * width * ff, bytes_accessed=6 * experts * width * ff,
                                      transcendentals=0),
        name="mlp",
    )(tiles, packed_one, packed_two, w_gate, w_up, w_down)


def mix_kernel(columns, starts_at, capacity, start_ref, base_ref, pos_ref, gate_ref, *rest):
    piece_refs, (out_ref, held_ref, sem) = rest[:-3], rest[-3:]
    step = pl.program_id(0)
    steps = pl.num_programs(0)
    width = base_ref.shape[1]

    @pl.when(step == 0)
    def _():
        copies = []
        for n, piece in enumerate(piece_refs):
            first, at = starts_at[n]
            experts, rows = piece.shape[:2]
            copies.append(pltpu.make_async_copy(
                piece, held_ref.at[pl.ds(first, experts), pl.ds(at, rows), :], sem.at[n]))
        for copy in copies:
            copy.start()
        for copy in copies:
            copy.wait()

    lane = lax.broadcasted_iota(I32, (MIX_ROWS, MIX_WIN), 1)
    bases, onehots, gates = [], [], []
    for column in columns:
        begin = start_ref[column * (steps + 1) + step]
        base = pl.multiple_of(jnp.minimum((begin // 16) * 16, capacity - MIX_WIN), 16)
        bases.append(base)
        onehots.append((pos_ref[:, column:column + 1] - base == lane).astype(F32).astype(BF16))
        gates.append(gate_ref[:, column:column + 1])
    for lo in range(0, width, MIX_COLS):
        cols = slice(lo, lo + MIX_COLS)
        total = base_ref[:, cols].astype(F32)
        for n in range(len(columns)):
            picked = jnp.dot(onehots[n], held_ref[n, pl.ds(bases[n], MIX_WIN), cols], preferred_element_type=F32)
            total = total + gates[n] * picked
        out_ref[:, cols] = total.astype(out_ref.dtype)


def mix_call(columns, starts_at, capacity, starts, base, pos, gates, pieces, out_dtype):
    tokens, width = base.shape
    block = pl.BlockSpec((MIX_ROWS, width), lambda i, s: (i, 0))
    small = pl.BlockSpec((MIX_ROWS, pos.shape[1]), lambda i, s: (i, 0))
    return pl.pallas_call(
        functools.partial(mix_kernel, columns, starts_at, capacity),
        grid_spec=pltpu.PrefetchScalarGridSpec(
            num_scalar_prefetch=1,
            grid=(tokens // MIX_ROWS,),
            in_specs=[block, small, small] + [pl.BlockSpec(memory_space=pl.ANY)] * len(pieces),
            out_specs=block,
            scratch_shapes=[pltpu.VMEM((len(columns), capacity, width), BF16), pltpu.SemaphoreType.DMA((len(pieces),))],
        ),
        out_shape=jax.ShapeDtypeStruct((tokens, width), out_dtype),
        compiler_params=pltpu.CompilerParams(vmem_limit_bytes=VMEM_LIMIT),
        cost_estimate=pl.CostEstimate(flops=2 * tokens * MIX_WIN * width * len(columns),
                                      bytes_accessed=tokens * width * 10, transcendentals=0),
        name="mix",
    )(starts, base, pos, gates, *pieces)


def solution(mesh):
    group_size = mesh.shape["ep"]
    rows_spec = P(("dp", "ep"))

    def swap(array, distance):
        return lax.ppermute(array, "ep", [(i, i ^ distance) for i in range(group_size)])

    def device_step(hidden, ln_gamma, ln_beta, w_router, w_gate, w_up, w_down, choice, mask_first, mask_second):
        tokens, _ = hidden.shape
        local = w_gate.shape[0]
        experts = local * group_size
        capacity = (10 * tokens + 4 * experts - 1) // (4 * experts)

        choice_t = choice.T
        rel_t = choice_t ^ (local * lax.axis_index("ep"))
        ids = lax.broadcasted_iota(I32, (experts, 1), 0)
        hit = ((rel_t[0:1] == ids) | (rel_t[1:2] == ids)).astype(I32)
        through = jnp.cumsum(hit, axis=1)
        before = through - hit
        pos = jnp.where((hit > 0) & (before < capacity), before, -1)
        starts = jnp.minimum(jnp.concatenate([before[:, ::MIX_ROWS], through[:, -1:]], axis=1), capacity)
        pack_starts = starts[:, ::PACK_ROWS // MIX_ROWS]
        marks = pack_starts.shape[1]
        meta = jnp.concatenate([pos, jnp.pad(pack_starts, ((0, 0), (0, 128 - marks)))], axis=1)
        metas = [meta[:local]] + [swap(meta[local * m:local * (m + 1)], m) for m in range(1, group_size)]

        halves = []
        for part in range(2):
            halves.append(norm_call(part, 2, hidden, ln_gamma[None], ln_beta[None]))

        sources = [halves, [swap(u, 1) for u in halves],
                   [swap(u, 2) for u in halves]]
        sources.append([swap(u, 1) for u in sources[2]])

        def pack(m):
            return pack_call(metas[m][:, tokens:tokens + marks].reshape(-1), metas[m][:, :tokens], *sources[m], capacity)

        def run(m_one, m_two, begin, rows, packed):
            most = jnp.maximum(metas[m_one][:, tokens + marks - 1], metas[m_two][:, tokens + marks - 1])
            tiles = jnp.clip((most - begin + TILE - 1) // TILE, 0, rows // TILE)
            return mlp_call(rows, begin // rows, tiles, *packed, w_gate, w_up, w_down)

        early = capacity - TILE
        near = [pack(0), pack(1)]
        near_early = run(0, 1, 0, early, near)
        home_early = swap(near_early[1], 1)

        far = [pack(2), pack(3)]
        far_rows = []
        for c in range(capacity // TILE):
            one, two = run(2, 3, c * TILE, TILE, far)
            far_rows.append((swap(one, 2), swap(two, 3)))

        near_late = run(0, 1, early, TILE, near)
        home_late = swap(near_late[1], 1)

        gates = [gate_call(part, u, w_router.T, choice_t, rel_t, mask_first.T, mask_second.T)
                 for part, u in enumerate(halves)]
        gates_t = jnp.concatenate(gates, axis=1).T
        pos_t = pos.T

        flat = starts.reshape(-1)
        total = mix_call(tuple(range(2 * local)), ((0, 0), (0, early), (local, 0), (local, early)), capacity, flat,
                         hidden, pos_t, gates_t, (near_early[0], near_late[0], home_early, home_late), F32)
        starts_at = tuple((local * n, c * TILE) for c in range(capacity // TILE) for n in range(2))
        return mix_call(tuple(range(2 * local, experts)), starts_at, capacity, flat, total, pos_t, gates_t,
                        tuple(piece for pair in far_rows for piece in pair), BF16)

    return jax.shard_map(device_step, mesh=mesh,
                         in_specs=(rows_spec, P(), P(), P(), P("ep"), P("ep"), P("ep"), rows_spec, rows_spec, rows_spec),
                         out_specs=rows_spec, check_vma=False)
```

```python
import functools

import jax
import jax.numpy as jnp
from jax import lax
from jax.experimental import pallas as pl
from jax.experimental.pallas import tpu as pltpu
from jax.sharding import PartitionSpec as P


LN_EPS = 1e-5
F32, BF16, I32 = jnp.float32, jnp.bfloat16, jnp.int32
VMEM_LIMIT = 67043328
NORM_ROWS = 256
NORM_GROUP = 16
GATE_ROWS = 512
PACK_ROWS = 512
PACK_WIN = 128
TILE = 160
FF_BLOCK = 1280
FF_SPLIT = 768
MIX_ROWS = 256
MIX_WIN = 256
WIDE_WIN = 272
LANES = 128
MIX_COLS = 256


def route_kernel(capacity, first_ref, choice_ref, table_ref, rel_ref, *meta_refs):
    experts = table_ref.shape[0]
    tokens = choice_ref.shape[1]
    rows = meta_refs[0].shape[0]
    rel = choice_ref[...] ^ first_ref[0]
    rel_ref[...] = rel
    ids = lax.broadcasted_iota(I32, (experts, LANES), 0)
    lane = lax.broadcasted_iota(I32, (experts, LANES), 1)
    earlier = (lax.broadcasted_iota(I32, (LANES, LANES), 0) < lax.broadcasted_iota(I32, (LANES, LANES), 1))
    earlier = earlier.astype(F32).astype(BF16)
    carry = jnp.zeros((experts, 1), F32)
    marks = jnp.zeros((experts, LANES), F32)

    def store(block, lo):
        table_ref[:, lo:lo + LANES] = block
        for m, ref in enumerate(meta_refs):
            ref[:, lo:lo + LANES] = block[m * rows:(m + 1) * rows, :]

    for n in range(tokens // LANES):
        lo = n * LANES
        hit = ((rel[0:1, lo:lo + LANES] == ids) | (rel[1:2, lo:lo + LANES] == ids)).astype(F32)
        before = jnp.dot(hit.astype(BF16), earlier, preferred_element_type=F32) + carry
        kept = (hit > 0) & (before < capacity)
        store(jnp.where(kept, before, -1.0).astype(I32), lo)
        marks = jnp.where(lane == n, carry, marks)
        carry = carry + jnp.sum(hit, axis=1, keepdims=True)
    marks = jnp.where(lane == tokens // LANES, carry, marks)
    store(jnp.minimum(marks, float(capacity)).astype(I32), tokens)


def route_call(first, choice_t, experts, local, capacity):
    tokens = choice_t.shape[1]
    table = lambda n: jax.ShapeDtypeStruct((n, tokens + LANES), I32)
    return pl.pallas_call(
        functools.partial(route_kernel, capacity),
        in_specs=[pl.BlockSpec(memory_space=pltpu.SMEM), pl.BlockSpec(memory_space=pltpu.VMEM)],
        out_specs=[pl.BlockSpec(memory_space=pltpu.VMEM)] * (2 + experts // local),
        out_shape=[table(experts), jax.ShapeDtypeStruct((2, tokens), I32)] + [table(local)] * (experts // local),
        cost_estimate=pl.CostEstimate(flops=1 << 24, bytes_accessed=1 << 18, transcendentals=0),
        name="route",
    )(first, choice_t)


def norm_kernel(x_ref, gamma_ref, beta_ref, u_ref):
    gamma = gamma_ref[...][None, :]
    beta = beta_ref[...][None, :]

    def group(n, carry):
        rows = pl.ds(pl.multiple_of(n * NORM_GROUP, NORM_GROUP), NORM_GROUP)
        values = x_ref[rows, :].astype(F32)
        centred = values - jnp.mean(values, axis=-1, keepdims=True)
        variance = jnp.mean(centred * centred, axis=-1, keepdims=True)
        u_ref[rows, :] = (centred * lax.rsqrt(variance + LN_EPS) * gamma + beta).astype(BF16)
        return carry

    lax.fori_loop(0, x_ref.shape[0] // NORM_GROUP, group, 0, unroll=4)


def norm_call(part, parts, hidden, gamma, beta):
    tokens, width = hidden.shape
    rows = tokens // parts
    steps = rows // NORM_ROWS
    vector = pl.BlockSpec((width,), lambda i: (0,))
    return pl.pallas_call(
        norm_kernel,
        grid=(steps,),
        in_specs=[pl.BlockSpec((NORM_ROWS, width), lambda i: (i + part * steps, 0)), vector, vector],
        out_specs=pl.BlockSpec((NORM_ROWS, width), lambda i: (i, 0)),
        out_shape=jax.ShapeDtypeStruct((rows, width), BF16),
        compiler_params=pltpu.CompilerParams(vmem_limit_bytes=VMEM_LIMIT),
        cost_estimate=pl.CostEstimate(flops=rows * width * 60, bytes_accessed=rows * width * 4, transcendentals=0),
        name="norm",
    )(hidden, gamma, beta)


def gate_kernel(u_ref, router_ref, choice_ref, rel_ref, first_ref, second_ref, gate_ref):
    scores = lax.dot_general(router_ref[...], u_ref[...], (((1,), (1,)), ((), ())), preferred_element_type=F32)
    expert_ids = lax.broadcasted_iota(I32, scores.shape, 0)
    gates = jnp.zeros_like(scores)
    for j, mask_ref in enumerate((first_ref, second_ref)):
        masked = jnp.where(mask_ref[...] > 0, scores, -jnp.inf)
        weights = jnp.exp(masked - jnp.max(masked, axis=0, keepdims=True))
        picked = jnp.where(expert_ids == choice_ref[j:j + 1, :], weights, 0.0)
        gate = jnp.sum(picked, axis=0, keepdims=True) / jnp.sum(weights, axis=0, keepdims=True)
        gates = gates + jnp.where(expert_ids == rel_ref[j:j + 1, :], gate, 0.0)
    gate_ref[...] = gates


def gate_call(part, u, router_t, choice_t, rel_t, first_t, second_t):
    rows, width = u.shape
    experts = router_t.shape[0]
    steps = rows // GATE_ROWS
    lanes = lambda n: pl.BlockSpec((n, GATE_ROWS), lambda i: (0, i + part * steps))
    return pl.pallas_call(
        gate_kernel,
        grid=(steps,),
        in_specs=[pl.BlockSpec((GATE_ROWS, width), lambda i: (i, 0)), pl.BlockSpec((experts, width), lambda i: (0, 0)),
                  lanes(2), lanes(2), lanes(experts), lanes(experts)],
        out_specs=pl.BlockSpec((experts, GATE_ROWS), lambda i: (0, i)),
        out_shape=jax.ShapeDtypeStruct((experts, rows), F32),
        compiler_params=pltpu.CompilerParams(vmem_limit_bytes=VMEM_LIMIT),
        cost_estimate=pl.CostEstimate(flops=rows * width * 60, bytes_accessed=rows * width * 2, transcendentals=0),
        name="gate",
    )(u, router_t, choice_t, rel_t, first_t, second_t)


def mark(tokens, rows, block):
    return tokens + block * (rows // LANES)


def pack_kernel(half_steps, meta_ref, pos_ref, low_ref, high_ref, rows_ref):
    step = pl.program_id(0)
    experts = rows_ref.shape[0]
    tokens = 2 * half_steps * PACK_ROWS

    @pl.when(step == 0)
    def _():
        rows_ref[...] = jnp.zeros_like(rows_ref)

    def pack(block_ref):
        for e in range(experts):
            begin = meta_ref[e, mark(tokens, PACK_ROWS, step)]
            end = meta_ref[e, mark(tokens, PACK_ROWS, step + 1)]
            base = (begin // 16) * 16
            windows = jnp.where(end > begin, (end - base + PACK_WIN - 1) // PACK_WIN, 0)
            slots = jnp.broadcast_to(pos_ref[e:e + 1, :], (PACK_WIN, PACK_ROWS))
            sublane = lax.broadcasted_iota(I32, (PACK_WIN, PACK_ROWS), 0)

            def window(w, carry):
                at = pl.multiple_of(base + w * PACK_WIN, 16)
                onehot = (slots - at == sublane).astype(F32).astype(BF16)
                picked = jnp.dot(onehot, block_ref[...], preferred_element_type=F32)
                held = rows_ref[e, pl.ds(at, PACK_WIN), :]
                rows_ref[e, pl.ds(at, PACK_WIN), :] = (held.astype(F32) + picked).astype(BF16)
                return carry

            lax.fori_loop(0, windows, window, 0)

    pl.when(step < half_steps)(lambda: pack(low_ref))
    pl.when(step >= half_steps)(lambda: pack(high_ref))


def pack_call(meta, low, high, capacity):
    half, width = low.shape
    experts = meta.shape[0]
    half_steps = half // PACK_ROWS
    padded = (capacity + PACK_WIN - 1) // PACK_WIN * PACK_WIN + PACK_WIN
    return pl.pallas_call(
        functools.partial(pack_kernel, half_steps),
        grid_spec=pltpu.PrefetchScalarGridSpec(
            num_scalar_prefetch=1,
            grid=(2 * half_steps,),
            in_specs=[pl.BlockSpec((experts, PACK_ROWS), lambda i, s: (0, i)),
                      pl.BlockSpec((PACK_ROWS, width), lambda i, s: (jnp.minimum(i, half_steps - 1), 0)),
                      pl.BlockSpec((PACK_ROWS, width), lambda i, s: (jnp.maximum(i - half_steps, 0), 0))],
            out_specs=pl.BlockSpec((experts, padded, width), lambda i, s: (0, 0, 0)),
        ),
        out_shape=jax.ShapeDtypeStruct((experts, padded, width), BF16),
        compiler_params=pltpu.CompilerParams(vmem_limit_bytes=VMEM_LIMIT),
        cost_estimate=pl.CostEstimate(flops=experts * 2 * half * PACK_ROWS * width, bytes_accessed=4 * half * width * 3,
                                      transcendentals=0),
        name="pack",
    )(meta, meta, low, high)


def row_tiles(begin, rows, tokens, expert, one_meta_ref, two_meta_ref):
    last = mark(tokens, tokens, 1)
    most = jnp.maximum(one_meta_ref[expert, last], two_meta_ref[expert, last])
    return jnp.clip((most - begin + TILE - 1) // TILE, 0, rows // TILE)


def tail_step(expert, step, steps):
    return step == jnp.where(expert % 2 == 0, 0, steps - 1)


def mlp_kernel(begin, tokens, splits, tail_splits, one_meta_ref, two_meta_ref, one_ref, two_ref, gate_ref, up_ref, down_ref, out_one_ref, out_two_ref, acc_ref):
    expert, step, steps = pl.program_id(0), pl.program_id(1), pl.num_programs(1)
    rows = out_one_ref.shape[1]
    tiles = row_tiles(begin, rows, tokens, expert, one_meta_ref, two_meta_ref)
    is_tail = tail_step(expert, step, steps)

    def accumulate(parts):
        def tile(i, carry):
            at = pl.multiple_of(i * TILE, TILE)
            both = pl.ds(pl.multiple_of(i * 2 * TILE, 2 * TILE), 2 * TILE)
            taken = jnp.concatenate([one_ref[0, pl.ds(at, TILE), :], two_ref[0, pl.ds(at, TILE), :]], axis=0)
            projs = []
            for lo, hi in parts:
                joined = jnp.concatenate([gate_ref[0, :, lo:hi], up_ref[0, :, lo:hi]], axis=1)
                projs.append(jnp.dot(taken, joined, preferred_element_type=F32))
            for n, (lo, hi) in enumerate(parts):
                inner = (jax.nn.silu(projs[n][:, :hi - lo]) * projs[n][:, hi - lo:]).astype(BF16)
                down = jnp.dot(inner, down_ref[0, lo:hi, :], preferred_element_type=F32)
                held = acc_ref[both, :]
                if n == 0:
                    held = jnp.where(step == 0, 0.0, held)
                acc_ref[both, :] = held + down
            return carry

        lax.fori_loop(0, tiles, tile, 0)

    pl.when(is_tail)(lambda: accumulate(tail_splits))
    pl.when(jnp.logical_not(is_tail))(lambda: accumulate(splits))

    @pl.when(step == steps - 1)
    def _():
        for i in range(rows // TILE):
            outs = [(ref, (2 * i + n) * TILE) for n, ref in enumerate((out_one_ref, out_two_ref))]

            @pl.when(i < tiles)
            def _():
                for ref, at in outs:
                    ref[0, i * TILE:(i + 1) * TILE, :] = acc_ref[at:at + TILE, :].astype(BF16)

            @pl.when(i >= tiles)
            def _():
                for ref, _at in outs:
                    ref[0, i * TILE:(i + 1) * TILE, :] = jnp.zeros((TILE, ref.shape[2]), BF16)


def mlp_call(tokens, begin, rows, meta_one, meta_two, packed_one, packed_two, w_gate, w_up, w_down):
    experts, width, ff = w_gate.shape
    full_steps, tail = divmod(ff, FF_BLOCK)
    splits = ((0, FF_SPLIT), (FF_SPLIT, FF_BLOCK))
    tail_splits = ((0, tail),)
    once = pl.Buffered(1)

    def block(e, f, one, two):
        idle = row_tiles(begin, rows, tokens, e, one, two) == 0
        return jnp.where(tail_step(e, f, full_steps + 1) | idle, full_steps, jnp.where(e % 2 == 0, f - 1, f))

    packed_spec = pl.BlockSpec((1, rows, width), lambda e, f, one, two: (e, begin // rows, 0), pipeline_mode=once)
    out_spec = pl.BlockSpec((1, rows, width), lambda e, f, one, two: (e, 0, 0), pipeline_mode=once)
    in_spec = pl.BlockSpec((1, width, FF_BLOCK), lambda e, f, one, two: (e, 0, block(e, f, one, two)))
    out = jax.ShapeDtypeStruct((experts, rows, width), BF16)
    return pl.pallas_call(
        functools.partial(mlp_kernel, begin, tokens, splits, tail_splits),
        grid_spec=pltpu.PrefetchScalarGridSpec(
            num_scalar_prefetch=2,
            grid=(experts, full_steps + 1),
            in_specs=[packed_spec, packed_spec, in_spec, in_spec,
                      pl.BlockSpec((1, FF_BLOCK, width), lambda e, f, one, two: (e, block(e, f, one, two), 0))],
            out_specs=[out_spec, out_spec],
            scratch_shapes=[pltpu.VMEM((2 * rows, width), F32)],
        ),
        out_shape=[out, out],
        compiler_params=pltpu.CompilerParams(vmem_limit_bytes=VMEM_LIMIT),
        cost_estimate=pl.CostEstimate(flops=6 * 2 * experts * rows * width * ff, bytes_accessed=6 * experts * width * ff,
                                      transcendentals=0),
        name="mlp",
    )(meta_one, meta_two, packed_one, packed_two, w_gate, w_up, w_down)


def mix_kernel(columns, starts_at, capacity, start_ref, base_ref, pos_ref, gate_ref, *rest):
    piece_refs, (out_ref, held_ref, sem) = rest[:-3], rest[-3:]
    step = pl.program_id(0)
    width = base_ref.shape[1]

    @pl.when(step == 0)
    def _():
        copies = []
        for n, piece in enumerate(piece_refs):
            first, at = starts_at[n]
            experts, rows = piece.shape[:2]
            copies.append(pltpu.make_async_copy(
                piece, held_ref.at[pl.ds(first, experts), pl.ds(at, rows), :], sem.at[n]))
        for copy in copies:
            copy.start()
        for copy in copies:
            copy.wait()

    def spans(window):
        for column in columns:
            begin = start_ref[column, step * (MIX_ROWS // LANES)]
            end = start_ref[column, (step + 1) * (MIX_ROWS // LANES)]
            base = pl.multiple_of(jnp.minimum((begin // 16) * 16, capacity - window), 16)
            yield base, end - base

    def mix(window):
        lane = lax.broadcasted_iota(I32, (MIX_ROWS, window), 1)
        bases = [base for base, _ in spans(window)]
        onehots = [(pos_ref[:, column:column + 1] - base == lane).astype(F32).astype(BF16)
                   for column, base in zip(columns, bases)]
        gates = [gate_ref[:, column:column + 1] for column in columns]
        for lo in range(0, width, MIX_COLS):
            cols = slice(lo, lo + MIX_COLS)
            total = base_ref[:, cols].astype(F32)
            for n in range(len(columns)):
                picked = jnp.dot(onehots[n], held_ref[n, pl.ds(bases[n], window), cols], preferred_element_type=F32)
                total = total + gates[n] * picked
            out_ref[:, cols] = total.astype(out_ref.dtype)

    fits = functools.reduce(jnp.logical_and, [rows <= MIX_WIN for _, rows in spans(MIX_WIN)])
    pl.when(fits)(lambda: mix(MIX_WIN))
    pl.when(jnp.logical_not(fits))(lambda: mix(WIDE_WIN))


def mix_call(columns, starts_at, capacity, starts, base, pos, gates, pieces, out_dtype):
    tokens, width = base.shape
    block = pl.BlockSpec((MIX_ROWS, width), lambda i, s: (i, 0))
    small = pl.BlockSpec((MIX_ROWS, pos.shape[1]), lambda i, s: (i, 0))
    return pl.pallas_call(
        functools.partial(mix_kernel, columns, starts_at, capacity),
        grid_spec=pltpu.PrefetchScalarGridSpec(
            num_scalar_prefetch=1,
            grid=(tokens // MIX_ROWS,),
            in_specs=[block, small, small] + [pl.BlockSpec(memory_space=pl.ANY)] * len(pieces),
            out_specs=block,
            scratch_shapes=[pltpu.VMEM((len(columns), capacity, width), BF16), pltpu.SemaphoreType.DMA((len(pieces),))],
        ),
        out_shape=jax.ShapeDtypeStruct((tokens, width), out_dtype),
        compiler_params=pltpu.CompilerParams(vmem_limit_bytes=VMEM_LIMIT),
        cost_estimate=pl.CostEstimate(flops=2 * tokens * MIX_WIN * width * len(columns),
                                      bytes_accessed=tokens * width * 10, transcendentals=0),
        name="mix",
    )(starts, base, pos, gates, *pieces)


def solution(mesh):
    group_size = mesh.shape["ep"]
    rows_spec = P(("dp", "ep"))

    def swap(array, distance):
        return lax.ppermute(array, "ep", [(i, i ^ distance) for i in range(group_size)])

    def device_step(hidden, ln_gamma, ln_beta, w_router, w_gate, w_up, w_down, choice, mask_first, mask_second):
        tokens, _ = hidden.shape
        local = w_gate.shape[0]
        experts = local * group_size
        capacity = (10 * tokens + 4 * experts - 1) // (4 * experts)

        choice_t = choice.T
        first = (local * lax.axis_index("ep")).astype(I32)[None]
        table, rel_t, *metas = route_call(first, choice_t, experts, local, capacity)
        metas = [metas[0]] + [swap(metas[m], m) for m in range(1, group_size)]

        halves = []
        for part in range(2):
            halves.append(norm_call(part, 2, hidden, ln_gamma, ln_beta))

        sources = [halves, [swap(u, 1) for u in halves],
                   [swap(u, 2) for u in halves]]
        sources.append([swap(u, 1) for u in sources[2]])

        def pack(m):
            return pack_call(metas[m], *sources[m], capacity)

        def run(m_one, m_two, begin, rows, packed):
            return mlp_call(tokens, begin, rows, metas[m_one], metas[m_two], *packed, w_gate, w_up, w_down)

        early = capacity - TILE
        near = [pack(0), pack(1)]
        near_early = run(0, 1, 0, early, near)
        home_early = swap(near_early[1], 1)

        far = [pack(2), pack(3)]
        far_rows = []
        for c in range(capacity // TILE):
            one, two = run(2, 3, c * TILE, TILE, far)
            far_rows.append((swap(one, 2), swap(two, 3)))

        near_late = run(0, 1, early, TILE, near)
        home_late = swap(near_late[1], 1)

        gates = [gate_call(part, u, w_router.T, choice_t, rel_t, mask_first.T, mask_second.T)
                 for part, u in enumerate(halves)]
        gates_t = jnp.concatenate(gates, axis=1).T
        pos_t = table[:, :tokens].T
        marks = table[:, tokens:]
        total = mix_call(tuple(range(2 * local)), ((0, 0), (0, early), (local, 0), (local, early)), capacity, marks,
                         hidden, pos_t, gates_t, (near_early[0], near_late[0], home_early, home_late), F32)
        starts_at = tuple((local * n, c * TILE) for c in range(capacity // TILE) for n in range(2))
        return mix_call(tuple(range(2 * local, experts)), starts_at, capacity, marks, total, pos_t, gates_t,
                        tuple(piece for pair in far_rows for piece in pair), BF16)

    return jax.shard_map(device_step, mesh=mesh,
                         in_specs=(rows_spec, P(), P(), P(), P("ep"), P("ep"), P("ep"), rows_spec, rows_spec, rows_spec),
                         out_specs=rows_spec, check_vma=False)
```

```python
import functools

import jax
import jax.numpy as jnp
from jax import lax
from jax.experimental import pallas as pl
from jax.experimental.pallas import tpu as pltpu
from jax.sharding import PartitionSpec as P


LN_EPS = 1e-5
F32, BF16, I32 = jnp.float32, jnp.bfloat16, jnp.int32
VMEM_LIMIT = 67043328
NORM_ROWS = 256
GATE_ROWS = 512
PACK_ROWS = 512
PACK_WIN = 128
FAR_TILE = 160
NEAR_TILE = 240
LATE_TILE = 80
FF_BLOCK = 1280
FF_SPLIT = 768
MIX_ROWS = 512
MIX_WIN = 256
WIDE_WIN = 528
LANES = 128
MIX_COLS = 256


def route_kernel(capacity, first_ref, choice_ref, table_ref, rel_ref, *meta_refs):
    experts = table_ref.shape[0]
    tokens = choice_ref.shape[1]
    rows = meta_refs[0].shape[0]
    rel = choice_ref[...] ^ first_ref[0]
    rel_ref[...] = rel
    ids = lax.broadcasted_iota(I32, (experts, LANES), 0)
    lane = lax.broadcasted_iota(I32, (experts, LANES), 1)
    earlier = (lax.broadcasted_iota(I32, (LANES, LANES), 0) < lax.broadcasted_iota(I32, (LANES, LANES), 1))
    earlier = earlier.astype(F32).astype(BF16)
    carry = jnp.zeros((experts, 1), F32)
    marks = jnp.zeros((experts, LANES), F32)

    def store(block, lo):
        table_ref[:, lo:lo + LANES] = block
        for m, ref in enumerate(meta_refs):
            ref[:, lo:lo + LANES] = block[m * rows:(m + 1) * rows, :]

    for n in range(tokens // LANES):
        lo = n * LANES
        hit = ((rel[0:1, lo:lo + LANES] == ids) | (rel[1:2, lo:lo + LANES] == ids)).astype(F32)
        before = jnp.dot(hit.astype(BF16), earlier, preferred_element_type=F32) + carry
        kept = (hit > 0) & (before < capacity)
        store(jnp.where(kept, before, -1.0).astype(I32), lo)
        marks = jnp.where(lane == n, carry, marks)
        carry = carry + jnp.sum(hit, axis=1, keepdims=True)
    marks = jnp.where(lane == tokens // LANES, carry, marks)
    store(jnp.minimum(marks, float(capacity)).astype(I32), tokens)


def route_call(first, choice_t, experts, local, capacity):
    tokens = choice_t.shape[1]
    table = lambda n: jax.ShapeDtypeStruct((n, tokens + LANES), I32)
    return pl.pallas_call(
        functools.partial(route_kernel, capacity),
        in_specs=[pl.BlockSpec(memory_space=pltpu.SMEM), pl.BlockSpec(memory_space=pltpu.VMEM)],
        out_specs=[pl.BlockSpec(memory_space=pltpu.VMEM)] * (2 + experts // local),
        out_shape=[table(experts), jax.ShapeDtypeStruct((2, tokens), I32)] + [table(local)] * (experts // local),
        cost_estimate=pl.CostEstimate(flops=1 << 24, bytes_accessed=1 << 18, transcendentals=0),
        name="route",
    )(first, choice_t)


def norm_kernel(x_ref, gamma_ref, beta_ref, u_ref):
    values = x_ref[...].astype(F32)
    centred = values - jnp.mean(values, axis=-1, keepdims=True)
    variance = jnp.mean(centred * centred, axis=-1, keepdims=True)
    normed = centred * lax.rsqrt(variance + LN_EPS) * gamma_ref[...][None, :] + beta_ref[...][None, :]
    u_ref[...] = normed.astype(BF16)


def norm_call(part, parts, hidden, gamma, beta):
    tokens, width = hidden.shape
    rows = tokens // parts
    steps = rows // NORM_ROWS
    vector = pl.BlockSpec((width,), lambda i: (0,))
    return pl.pallas_call(
        norm_kernel,
        grid=(steps,),
        in_specs=[pl.BlockSpec((NORM_ROWS, width), lambda i: (i + part * steps, 0)), vector, vector],
        out_specs=pl.BlockSpec((NORM_ROWS, width), lambda i: (i, 0)),
        out_shape=jax.ShapeDtypeStruct((rows, width), BF16),
        compiler_params=pltpu.CompilerParams(vmem_limit_bytes=VMEM_LIMIT),
        cost_estimate=pl.CostEstimate(flops=rows * width * 60, bytes_accessed=rows * width * 4, transcendentals=0),
        name="norm",
    )(hidden, gamma, beta)


def gate_kernel(u_ref, router_ref, choice_ref, rel_ref, first_ref, second_ref, gate_ref):
    scores = lax.dot_general(router_ref[...], u_ref[...], (((1,), (1,)), ((), ())), preferred_element_type=F32)
    expert_ids = lax.broadcasted_iota(I32, scores.shape, 0)
    gates = jnp.zeros_like(scores)
    for j, mask_ref in enumerate((first_ref, second_ref)):
        masked = jnp.where(mask_ref[...] > 0, scores, -jnp.inf)
        weights = jnp.exp(masked - jnp.max(masked, axis=0, keepdims=True))
        picked = jnp.where(expert_ids == choice_ref[j:j + 1, :], weights, 0.0)
        gate = jnp.sum(picked, axis=0, keepdims=True) / jnp.sum(weights, axis=0, keepdims=True)
        gates = gates + jnp.where(expert_ids == rel_ref[j:j + 1, :], gate, 0.0)
    gate_ref[...] = gates


def gate_call(part, u, router_t, choice_t, rel_t, first_t, second_t):
    rows, width = u.shape
    experts = router_t.shape[0]
    steps = rows // GATE_ROWS
    lanes = lambda n: pl.BlockSpec((n, GATE_ROWS), lambda i: (0, i + part * steps))
    return pl.pallas_call(
        gate_kernel,
        grid=(steps,),
        in_specs=[pl.BlockSpec((GATE_ROWS, width), lambda i: (i, 0)), pl.BlockSpec((experts, width), lambda i: (0, 0)),
                  lanes(2), lanes(2), lanes(experts), lanes(experts)],
        out_specs=pl.BlockSpec((experts, GATE_ROWS), lambda i: (0, i)),
        out_shape=jax.ShapeDtypeStruct((experts, rows), F32),
        compiler_params=pltpu.CompilerParams(vmem_limit_bytes=VMEM_LIMIT),
        cost_estimate=pl.CostEstimate(flops=rows * width * 60, bytes_accessed=rows * width * 2, transcendentals=0),
        name="gate",
    )(u, router_t, choice_t, rel_t, first_t, second_t)


def mark(tokens, rows, block):
    return tokens + block * (rows // LANES)


def pack_kernel(half_steps, meta_ref, pos_ref, low_ref, high_ref, rows_ref):
    step = pl.program_id(0)
    experts = rows_ref.shape[0]
    tokens = 2 * half_steps * PACK_ROWS

    @pl.when(step == 0)
    def _():
        rows_ref[...] = jnp.zeros_like(rows_ref)

    def pack(block_ref):
        for e in range(experts):
            begin = meta_ref[e, mark(tokens, PACK_ROWS, step)]
            end = meta_ref[e, mark(tokens, PACK_ROWS, step + 1)]
            base = (begin // 16) * 16
            windows = jnp.where(end > begin, (end - base + PACK_WIN - 1) // PACK_WIN, 0)
            slots = jnp.broadcast_to(pos_ref[e:e + 1, :], (PACK_WIN, PACK_ROWS))
            sublane = lax.broadcasted_iota(I32, (PACK_WIN, PACK_ROWS), 0)

            def window(w, carry):
                at = pl.multiple_of(base + w * PACK_WIN, 16)
                onehot = (slots - at == sublane).astype(F32).astype(BF16)
                picked = jnp.dot(onehot, block_ref[...], preferred_element_type=F32)
                held = rows_ref[e, pl.ds(at, 16), :]
                rows_ref[e, pl.ds(at, 16), :] = (held.astype(F32) + picked[:16]).astype(BF16)
                rows_ref[e, pl.ds(pl.multiple_of(at + 16, 16), PACK_WIN - 16), :] = picked[16:].astype(BF16)
                return carry

            lax.fori_loop(0, windows, window, 0)

    pl.when(step < half_steps)(lambda: pack(low_ref))
    pl.when(step >= half_steps)(lambda: pack(high_ref))


def pack_call(meta, low, high, capacity):
    half, width = low.shape
    experts = meta.shape[0]
    half_steps = half // PACK_ROWS
    padded = (capacity + PACK_WIN - 1) // PACK_WIN * PACK_WIN + PACK_WIN
    return pl.pallas_call(
        functools.partial(pack_kernel, half_steps),
        grid_spec=pltpu.PrefetchScalarGridSpec(
            num_scalar_prefetch=1,
            grid=(2 * half_steps,),
            in_specs=[pl.BlockSpec((experts, PACK_ROWS), lambda i, s: (0, i)),
                      pl.BlockSpec((PACK_ROWS, width), lambda i, s: (jnp.minimum(i, half_steps - 1), 0)),
                      pl.BlockSpec((PACK_ROWS, width), lambda i, s: (jnp.maximum(i - half_steps, 0), 0))],
            out_specs=pl.BlockSpec((experts, padded, width), lambda i, s: (0, 0, 0)),
        ),
        out_shape=jax.ShapeDtypeStruct((experts, padded, width), BF16),
        compiler_params=pltpu.CompilerParams(vmem_limit_bytes=VMEM_LIMIT),
        cost_estimate=pl.CostEstimate(flops=experts * 2 * half * PACK_ROWS * width, bytes_accessed=4 * half * width * 3,
                                      transcendentals=0),
        name="pack",
    )(meta, meta, low, high)


def row_tiles(begin, rows, tile, tokens, expert, meta_refs):
    last = mark(tokens, tokens, 1)
    most = functools.reduce(jnp.maximum, [ref[expert, last] for ref in meta_refs])
    return jnp.clip((most - begin + tile - 1) // tile, 0, rows // tile)


def tail_step(turn, step, steps):
    return step == jnp.where(turn % 2 == 0, 0, steps - 1)


def mlp_kernel(begin, tile_rows, tokens, first_expert, splits, tail_splits, sources, *refs):
    meta_refs, row_refs = refs[:sources], refs[sources:2 * sources]
    gate_ref, up_ref, down_ref = refs[2 * sources:2 * sources + 3]
    out_refs, acc_ref = refs[2 * sources + 3:-1], refs[-1]
    turn, step, steps = pl.program_id(0), pl.program_id(1), pl.num_programs(1)
    rows = out_refs[0].shape[1]
    height = sources * tile_rows
    tiles = row_tiles(begin, rows, tile_rows, tokens, first_expert + turn, meta_refs)
    is_tail = tail_step(turn, step, steps)

    def accumulate(parts):
        def tile(i, carry):
            at = pl.multiple_of(i * tile_rows, tile_rows)
            held_rows = pl.ds(pl.multiple_of(i * height, height), height)
            taken = jnp.concatenate([ref[0, pl.ds(at, tile_rows), :] for ref in row_refs], axis=0)
            projs = []
            for lo, hi in parts:
                joined = jnp.concatenate([gate_ref[0, :, lo:hi], up_ref[0, :, lo:hi]], axis=1)
                projs.append(jnp.dot(taken, joined, preferred_element_type=F32))
            for n, (lo, hi) in enumerate(parts):
                inner = (jax.nn.silu(projs[n][:, :hi - lo]) * projs[n][:, hi - lo:]).astype(BF16)
                down = jnp.dot(inner, down_ref[0, lo:hi, :], preferred_element_type=F32)
                held = acc_ref[held_rows, :]
                if n == 0:
                    held = jnp.where(step == 0, 0.0, held)
                acc_ref[held_rows, :] = held + down
            return carry

        lax.fori_loop(0, tiles, tile, 0)

    pl.when(is_tail)(lambda: accumulate(tail_splits))
    pl.when(jnp.logical_not(is_tail))(lambda: accumulate(splits))

    @pl.when(step == steps - 1)
    def _():
        for i in range(rows // tile_rows):
            @pl.when(i < tiles)
            def _():
                for n, ref in enumerate(out_refs):
                    at = (sources * i + n) * tile_rows
                    ref[0, i * tile_rows:(i + 1) * tile_rows, :] = acc_ref[at:at + tile_rows, :].astype(BF16)

            @pl.when(i >= tiles)
            def _():
                for ref in out_refs:
                    ref[0, i * tile_rows:(i + 1) * tile_rows, :] = jnp.zeros((tile_rows, ref.shape[2]), BF16)


def mlp_call(tokens, begin, rows, tile_rows, first_expert, experts, metas, packed, w_gate, w_up, w_down):
    width, ff = w_gate.shape[1:]
    sources = len(metas)
    full_steps, tail = divmod(ff, FF_BLOCK)
    splits = ((0, FF_SPLIT), (FF_SPLIT, FF_BLOCK))
    tail_splits = ((0, tail),)
    once = pl.Buffered(1)

    def block(e, f, refs):
        idle = row_tiles(begin, rows, tile_rows, tokens, first_expert + e, refs) == 0
        return jnp.where(tail_step(e, f, full_steps + 1) | idle, full_steps, jnp.where(e % 2 == 0, f - 1, f))

    packed_spec = pl.BlockSpec((1, rows, width), lambda e, f, *m: (first_expert + e, begin // rows, 0), pipeline_mode=once)
    out_spec = pl.BlockSpec((1, rows, width), lambda e, f, *m: (e, 0, 0), pipeline_mode=once)
    in_spec = pl.BlockSpec((1, width, FF_BLOCK), lambda e, f, *m: (first_expert + e, 0, block(e, f, m)))
    down_spec = pl.BlockSpec((1, FF_BLOCK, width), lambda e, f, *m: (first_expert + e, block(e, f, m), 0))
    out = jax.ShapeDtypeStruct((experts, rows, width), BF16)
    return pl.pallas_call(
        functools.partial(mlp_kernel, begin, tile_rows, tokens, first_expert, splits, tail_splits, sources),
        grid_spec=pltpu.PrefetchScalarGridSpec(
            num_scalar_prefetch=sources,
            grid=(experts, full_steps + 1),
            in_specs=[packed_spec] * sources + [in_spec, in_spec, down_spec],
            out_specs=[out_spec] * sources,
            scratch_shapes=[pltpu.VMEM((sources * rows, width), F32)],
        ),
        out_shape=[out] * sources,
        compiler_params=pltpu.CompilerParams(vmem_limit_bytes=VMEM_LIMIT),
        cost_estimate=pl.CostEstimate(flops=6 * sources * experts * rows * width * ff,
                                      bytes_accessed=6 * experts * width * ff, transcendentals=0),
        name="mlp",
    )(*metas, *packed, w_gate, w_up, w_down)


def mix_kernel(columns, starts_at, capacity, start_ref, base_ref, pos_ref, gate_ref, *rest):
    piece_refs, (out_ref, held_ref, sem) = rest[:-3], rest[-3:]
    step = pl.program_id(0)
    width = base_ref.shape[1]

    @pl.when(step == 0)
    def _():
        copies = []
        for n, piece in enumerate(piece_refs):
            first, at = starts_at[n]
            experts, rows = piece.shape[:2]
            copies.append(pltpu.make_async_copy(
                piece, held_ref.at[pl.ds(first, experts), pl.ds(at, rows), :], sem.at[n]))
        for copy in copies:
            copy.start()
        for copy in copies:
            copy.wait()

    def spans(window):
        for column in columns:
            begin = start_ref[column, step * (MIX_ROWS // LANES)]
            end = start_ref[column, (step + 1) * (MIX_ROWS // LANES)]
            base = pl.multiple_of(jnp.minimum((begin // 16) * 16, capacity - window), 16)
            yield base, end - base

    def mix(window):
        lane = lax.broadcasted_iota(I32, (MIX_ROWS, window), 1)
        bases = [base for base, _ in spans(window)]
        onehots = [(pos_ref[:, column:column + 1] - base == lane).astype(F32).astype(BF16)
                   for column, base in zip(columns, bases)]
        gates = [gate_ref[:, column:column + 1] for column in columns]
        for lo in range(0, width, MIX_COLS):
            cols = slice(lo, lo + MIX_COLS)
            total = base_ref[:, cols].astype(F32)
            for n in range(len(columns)):
                picked = jnp.dot(onehots[n], held_ref[n, pl.ds(bases[n], window), cols], preferred_element_type=F32)
                total = total + gates[n] * picked
            out_ref[:, cols] = total.astype(out_ref.dtype)

    fits = functools.reduce(jnp.logical_and, [rows <= MIX_WIN for _, rows in spans(MIX_WIN)])
    pl.when(fits)(lambda: mix(MIX_WIN))
    pl.when(jnp.logical_not(fits))(lambda: mix(WIDE_WIN))


def mix_call(columns, capacity, starts, base, pos, gates, placed, out_dtype):
    starts_at, pieces = zip(*placed)
    tokens, width = base.shape
    block = pl.BlockSpec((MIX_ROWS, width), lambda i, s: (i, 0))
    small = pl.BlockSpec((MIX_ROWS, pos.shape[1]), lambda i, s: (i, 0))
    return pl.pallas_call(
        functools.partial(mix_kernel, columns, starts_at, capacity),
        grid_spec=pltpu.PrefetchScalarGridSpec(
            num_scalar_prefetch=1,
            grid=(tokens // MIX_ROWS,),
            in_specs=[block, small, small] + [pl.BlockSpec(memory_space=pl.ANY)] * len(pieces),
            out_specs=block,
            scratch_shapes=[pltpu.VMEM((len(columns), capacity, width), BF16), pltpu.SemaphoreType.DMA((len(pieces),))],
        ),
        out_shape=jax.ShapeDtypeStruct((tokens, width), out_dtype),
        compiler_params=pltpu.CompilerParams(vmem_limit_bytes=VMEM_LIMIT),
        cost_estimate=pl.CostEstimate(flops=2 * tokens * MIX_WIN * width * len(columns),
                                      bytes_accessed=tokens * width * 10, transcendentals=0),
        name="mix",
    )(starts, base, pos, gates, *pieces)


def solution(mesh):
    group_size = mesh.shape["ep"]
    rows_spec = P(("dp", "ep"))

    def swap(array, distance):
        return lax.ppermute(array, "ep", [(i, i ^ distance) for i in range(group_size)])

    def device_step(hidden, ln_gamma, ln_beta, w_router, w_gate, w_up, w_down, choice, mask_first, mask_second):
        tokens, _ = hidden.shape
        local = w_gate.shape[0]
        experts = local * group_size
        capacity = (10 * tokens + 4 * experts - 1) // (4 * experts)

        choice_t = choice.T
        first = (local * lax.axis_index("ep")).astype(I32)[None]
        table, rel_t, *metas = route_call(first, choice_t, experts, local, capacity)
        metas = [metas[0]] + [swap(metas[m], m) for m in range(1, group_size)]

        halves = []
        for part in range(2):
            halves.append(norm_call(part, 2, hidden, ln_gamma, ln_beta))

        sources = [halves, [swap(u, 1) for u in halves],
                   [swap(u, 2) for u in halves]]
        sources.append([swap(u, 1) for u in sources[2]])

        def pack(m):
            return pack_call(metas[m], *sources[m], capacity)

        packed = {}

        def run(places, begin, rows, tile_rows, first_expert=0, count=local):
            return mlp_call(tokens, begin, rows, tile_rows, first_expert, count, [metas[m] for m in places],
                            [packed[m] for m in places], w_gate, w_up, w_down)

        late = capacity - FAR_TILE
        packed[0], packed[1] = pack(0), pack(1)
        near_early = run((0, 1), 0, late, NEAR_TILE)
        near_rows = [((0, 0), near_early[0]), ((local, 0), swap(near_early[1], 1))]

        packed[2], packed[3] = pack(2), pack(3)
        far_rows = []

        def send_far(expert, at, two, three):
            far_rows.append(((expert, at), swap(two, 2)))
            far_rows.append(((local + expert, at), swap(three, 3)))

        for c in range(late // FAR_TILE - 1):
            send_far(0, c * FAR_TILE, *run((2, 3), c * FAR_TILE, FAR_TILE, FAR_TILE))
        zero, one, two, three = run((0, 1, 2, 3), late, FAR_TILE, LATE_TILE)
        send_far(0, late, two, three)
        near_rows += [((0, late), zero), ((local, late), swap(one, 1))]
        final = late - FAR_TILE
        for e in range(local):
            send_far(e, final, *run((2, 3), final, FAR_TILE, FAR_TILE, e, 1))

        gates = [gate_call(part, u, w_router.T, choice_t, rel_t, mask_first.T, mask_second.T)
                 for part, u in enumerate(halves)]
        gates_t = jnp.concatenate(gates, axis=1).T
        pos_t = table[:, :tokens].T
        marks = table[:, tokens:]
        total = mix_call(tuple(range(2 * local)), capacity, marks, hidden, pos_t, gates_t, near_rows, F32)
        return mix_call(tuple(range(2 * local, experts)), capacity, marks, total, pos_t, gates_t, far_rows, BF16)

    return jax.shard_map(device_step, mesh=mesh,
                         in_specs=(rows_spec, P(), P(), P(), P("ep"), P("ep"), P("ep"), rows_spec, rows_spec, rows_spec),
                         out_specs=rows_spec, check_vma=False)
```

```python
import functools

import jax
import jax.numpy as jnp
from jax import lax
from jax.experimental import pallas as pl
from jax.experimental.pallas import tpu as pltpu
from jax.sharding import PartitionSpec as P


LN_EPS = 1e-5
F32, BF16, I32 = jnp.float32, jnp.bfloat16, jnp.int32
VMEM_LIMIT = 67043328
NORM_ROWS = 256
GATE_ROWS = 512
PACK_ROWS = 256
PACK_WIN = 128
FAR_TILE = 192
NEAR_TILE = 256
LATE_TILE = 64
LATE_ROWS = 128
FF_BLOCK = 1280
FF_SPLIT = 768
MIX_ROWS = 512
MIX_WIN = 256
WIDE_WIN = 528
LANES = 128
MIX_COLS = 256


def route_kernel(capacity, first_ref, choice_ref, table_ref, rel_ref, *meta_refs):
    experts = table_ref.shape[0]
    tokens = choice_ref.shape[1]
    rows = meta_refs[0].shape[0]
    rel = choice_ref[...] ^ first_ref[0]
    rel_ref[...] = rel
    ids = lax.broadcasted_iota(I32, (experts, LANES), 0)
    lane = lax.broadcasted_iota(I32, (experts, LANES), 1)
    earlier = (lax.broadcasted_iota(I32, (LANES, LANES), 0) < lax.broadcasted_iota(I32, (LANES, LANES), 1))
    earlier = earlier.astype(F32).astype(BF16)
    carry = jnp.zeros((experts, 1), F32)
    marks = jnp.zeros((experts, LANES), F32)

    def store(block, lo):
        table_ref[:, lo:lo + LANES] = block
        for m, ref in enumerate(meta_refs):
            ref[:, lo:lo + LANES] = block[m * rows:(m + 1) * rows, :]

    for n in range(tokens // LANES):
        lo = n * LANES
        hit = ((rel[0:1, lo:lo + LANES] == ids) | (rel[1:2, lo:lo + LANES] == ids)).astype(F32)
        before = jnp.dot(hit.astype(BF16), earlier, preferred_element_type=F32) + carry
        kept = (hit > 0) & (before < capacity)
        store(jnp.where(kept, before, -1.0).astype(I32), lo)
        marks = jnp.where(lane == n, carry, marks)
        carry = carry + jnp.sum(hit, axis=1, keepdims=True)
    marks = jnp.where(lane == tokens // LANES, carry, marks)
    store(jnp.minimum(marks, float(capacity)).astype(I32), tokens)


def route_call(first, choice_t, experts, local, capacity):
    tokens = choice_t.shape[1]
    table = lambda n: jax.ShapeDtypeStruct((n, tokens + LANES), I32)
    return pl.pallas_call(
        functools.partial(route_kernel, capacity),
        in_specs=[pl.BlockSpec(memory_space=pltpu.SMEM), pl.BlockSpec(memory_space=pltpu.VMEM)],
        out_specs=[pl.BlockSpec(memory_space=pltpu.VMEM)] * (2 + experts // local),
        out_shape=[table(experts), jax.ShapeDtypeStruct((2, tokens), I32)] + [table(local)] * (experts // local),
        cost_estimate=pl.CostEstimate(flops=1 << 24, bytes_accessed=1 << 18, transcendentals=0),
        name="route",
    )(first, choice_t)


def norm_kernel(x_ref, gamma_ref, beta_ref, u_ref):
    values = x_ref[...].astype(F32)
    centred = values - jnp.mean(values, axis=-1, keepdims=True)
    variance = jnp.mean(centred * centred, axis=-1, keepdims=True)
    normed = centred * lax.rsqrt(variance + LN_EPS) * gamma_ref[...][None, :] + beta_ref[...][None, :]
    u_ref[...] = normed.astype(BF16)


def norm_call(part, parts, hidden, gamma, beta):
    tokens, width = hidden.shape
    rows = tokens // parts
    steps = rows // NORM_ROWS
    vector = pl.BlockSpec((width,), lambda i: (0,))
    return pl.pallas_call(
        norm_kernel,
        grid=(steps,),
        in_specs=[pl.BlockSpec((NORM_ROWS, width), lambda i: (i + part * steps, 0)), vector, vector],
        out_specs=pl.BlockSpec((NORM_ROWS, width), lambda i: (i, 0)),
        out_shape=jax.ShapeDtypeStruct((rows, width), BF16),
        compiler_params=pltpu.CompilerParams(vmem_limit_bytes=VMEM_LIMIT),
        cost_estimate=pl.CostEstimate(flops=rows * width * 60, bytes_accessed=rows * width * 4, transcendentals=0),
        name="norm",
    )(hidden, gamma, beta)


def gate_kernel(u_ref, router_ref, choice_ref, rel_ref, first_ref, second_ref, gate_ref):
    scores = lax.dot_general(router_ref[...], u_ref[...], (((1,), (1,)), ((), ())), preferred_element_type=F32)
    expert_ids = lax.broadcasted_iota(I32, scores.shape, 0)
    gates = jnp.zeros_like(scores)
    for j, mask_ref in enumerate((first_ref, second_ref)):
        masked = jnp.where(mask_ref[...] > 0, scores, -jnp.inf)
        weights = jnp.exp(masked - jnp.max(masked, axis=0, keepdims=True))
        picked = jnp.where(expert_ids == choice_ref[j:j + 1, :], weights, 0.0)
        gate = jnp.sum(picked, axis=0, keepdims=True) / jnp.sum(weights, axis=0, keepdims=True)
        gates = gates + jnp.where(expert_ids == rel_ref[j:j + 1, :], gate, 0.0)
    gate_ref[...] = gates


def gate_call(part, u, router_t, choice_t, rel_t, first_t, second_t):
    rows, width = u.shape
    experts = router_t.shape[0]
    steps = rows // GATE_ROWS
    lanes = lambda n: pl.BlockSpec((n, GATE_ROWS), lambda i: (0, i + part * steps))
    return pl.pallas_call(
        gate_kernel,
        grid=(steps,),
        in_specs=[pl.BlockSpec((GATE_ROWS, width), lambda i: (i, 0)), pl.BlockSpec((experts, width), lambda i: (0, 0)),
                  lanes(2), lanes(2), lanes(experts), lanes(experts)],
        out_specs=pl.BlockSpec((experts, GATE_ROWS), lambda i: (0, i)),
        out_shape=jax.ShapeDtypeStruct((experts, rows), F32),
        compiler_params=pltpu.CompilerParams(vmem_limit_bytes=VMEM_LIMIT),
        cost_estimate=pl.CostEstimate(flops=rows * width * 60, bytes_accessed=rows * width * 2, transcendentals=0),
        name="gate",
    )(u, router_t, choice_t, rel_t, first_t, second_t)


def mark(tokens, rows, block):
    return tokens + block * (rows // LANES)


def pack_kernel(half_steps, meta_ref, pos_ref, low_ref, high_ref, rows_ref):
    step = pl.program_id(0)
    experts = rows_ref.shape[0]
    tokens = 2 * half_steps * PACK_ROWS

    @pl.when(step == 0)
    def _():
        rows_ref[...] = jnp.zeros_like(rows_ref)

    def pack(block_ref):
        sublane = lax.broadcasted_iota(I32, (PACK_WIN, PACK_ROWS), 0)
        spans, slots = [], []
        for e in range(experts):
            begin = meta_ref[e, mark(tokens, PACK_ROWS, step)]
            base = (begin // 16) * 16
            spans.append((base, meta_ref[e, mark(tokens, PACK_ROWS, step + 1)] - base))
            slots.append(jnp.broadcast_to(pos_ref[e:e + 1, :], (PACK_WIN, PACK_ROWS)))

        def onehot(e, at):
            return (slots[e] - at == sublane).astype(F32)

        def put(e, at, picked):
            head, body = pl.ds(pl.multiple_of(at, 16), 16), pl.ds(pl.multiple_of(at + 16, 16), PACK_WIN - 16)
            rows_ref[e, head, :] = (rows_ref[e, head, :].astype(F32) + picked[:16]).astype(BF16)
            rows_ref[e, body, :] = picked[16:].astype(BF16)

        joined = jnp.concatenate([onehot(e, spans[e][0]) for e in range(experts)], axis=0).astype(BF16)
        picked = jnp.dot(joined, block_ref[...], preferred_element_type=F32)
        for e in range(experts):
            put(e, spans[e][0], picked[e * PACK_WIN:(e + 1) * PACK_WIN])

            def window(w, carry):
                at = spans[e][0] + w * PACK_WIN
                put(e, at, jnp.dot(onehot(e, at).astype(BF16), block_ref[...], preferred_element_type=F32))
                return carry

            lax.fori_loop(1, (spans[e][1] + PACK_WIN - 1) // PACK_WIN, window, 0)

    pl.when(step < half_steps)(lambda: pack(low_ref))
    pl.when(step >= half_steps)(lambda: pack(high_ref))


def pack_call(meta, low, high, capacity):
    half, width = low.shape
    experts = meta.shape[0]
    half_steps = half // PACK_ROWS
    padded = (capacity + PACK_WIN - 1) // PACK_WIN * PACK_WIN + PACK_WIN
    return pl.pallas_call(
        functools.partial(pack_kernel, half_steps),
        grid_spec=pltpu.PrefetchScalarGridSpec(
            num_scalar_prefetch=1,
            grid=(2 * half_steps,),
            in_specs=[pl.BlockSpec((experts, PACK_ROWS), lambda i, s: (0, i)),
                      pl.BlockSpec((PACK_ROWS, width), lambda i, s: (jnp.minimum(i, half_steps - 1), 0)),
                      pl.BlockSpec((PACK_ROWS, width), lambda i, s: (jnp.maximum(i - half_steps, 0), 0))],
            out_specs=pl.BlockSpec((experts, padded, width), lambda i, s: (0, 0, 0)),
        ),
        out_shape=jax.ShapeDtypeStruct((experts, padded, width), BF16),
        compiler_params=pltpu.CompilerParams(vmem_limit_bytes=VMEM_LIMIT),
        cost_estimate=pl.CostEstimate(flops=experts * 2 * half * PACK_ROWS * width, bytes_accessed=4 * half * width * 3,
                                      transcendentals=0),
        name="pack",
    )(meta, meta, low, high)


def row_tiles(begin, rows, tile, tokens, expert, meta_refs):
    last = mark(tokens, tokens, 1)
    most = functools.reduce(jnp.maximum, [ref[expert, last] for ref in meta_refs])
    return jnp.clip((most - begin + tile - 1) // tile, 0, rows // tile)


def tail_step(turn, step, steps):
    return step == jnp.where(turn % 2 == 0, 0, steps - 1)


def mlp_kernel(begin, tile_rows, tokens, first_expert, splits, tail_splits, sources, *refs):
    meta_refs, row_refs = refs[:sources], refs[sources:2 * sources]
    gate_ref, up_ref, down_ref = refs[2 * sources:2 * sources + 3]
    out_refs, acc_ref = refs[2 * sources + 3:-1], refs[-1]
    turn, step, steps = pl.program_id(0), pl.program_id(1), pl.num_programs(1)
    rows = out_refs[0].shape[1]
    height = sources * tile_rows
    tiles = row_tiles(begin, rows, tile_rows, tokens, first_expert + turn, meta_refs)
    is_tail = tail_step(turn, step, steps)

    def accumulate(parts):
        def tile(i, carry):
            at = pl.multiple_of(i * tile_rows, tile_rows)
            held_rows = pl.ds(pl.multiple_of(i * height, height), height)
            taken = jnp.concatenate([ref[0, pl.ds(at, tile_rows), :] for ref in row_refs], axis=0)
            projs = []
            for lo, hi in parts:
                joined = jnp.concatenate([gate_ref[0, :, lo:hi], up_ref[0, :, lo:hi]], axis=1)
                projs.append(jnp.dot(taken, joined, preferred_element_type=F32))
            for n, (lo, hi) in enumerate(parts):
                inner = (jax.nn.silu(projs[n][:, :hi - lo]) * projs[n][:, hi - lo:]).astype(BF16)
                down = jnp.dot(inner, down_ref[0, lo:hi, :], preferred_element_type=F32)
                held = acc_ref[held_rows, :]
                if n == 0:
                    held = jnp.where(step == 0, 0.0, held)
                acc_ref[held_rows, :] = held + down
            return carry

        lax.fori_loop(0, tiles, tile, 0)

    pl.when(is_tail)(lambda: accumulate(tail_splits))
    pl.when(jnp.logical_not(is_tail))(lambda: accumulate(splits))

    @pl.when(step == steps - 1)
    def _():
        for i in range(rows // tile_rows):
            @pl.when(i < tiles)
            def _():
                for n, ref in enumerate(out_refs):
                    at = (sources * i + n) * tile_rows
                    ref[0, i * tile_rows:(i + 1) * tile_rows, :] = acc_ref[at:at + tile_rows, :].astype(BF16)

            @pl.when(i >= tiles)
            def _():
                for ref in out_refs:
                    ref[0, i * tile_rows:(i + 1) * tile_rows, :] = jnp.zeros((tile_rows, ref.shape[2]), BF16)


def mlp_call(tokens, begin, rows, tile_rows, first_expert, experts, metas, packed, w_gate, w_up, w_down):
    width, ff = w_gate.shape[1:]
    sources = len(metas)
    full_steps, tail = divmod(ff, FF_BLOCK)
    splits = ((0, FF_SPLIT), (FF_SPLIT, FF_BLOCK))
    tail_splits = ((0, tail),)
    once = pl.Buffered(1)

    def block(e, f, refs):
        idle = row_tiles(begin, rows, tile_rows, tokens, first_expert + e, refs) == 0
        return jnp.where(tail_step(e, f, full_steps + 1) | idle, full_steps, jnp.where(e % 2 == 0, f - 1, f))

    packed_spec = pl.BlockSpec((1, rows, width), lambda e, f, *m: (first_expert + e, begin // rows, 0), pipeline_mode=once)
    out_spec = pl.BlockSpec((1, rows, width), lambda e, f, *m: (e, 0, 0), pipeline_mode=once)
    in_spec = pl.BlockSpec((1, width, FF_BLOCK), lambda e, f, *m: (first_expert + e, 0, block(e, f, m)))
    down_spec = pl.BlockSpec((1, FF_BLOCK, width), lambda e, f, *m: (first_expert + e, block(e, f, m), 0))
    out = jax.ShapeDtypeStruct((experts, rows, width), BF16)
    return pl.pallas_call(
        functools.partial(mlp_kernel, begin, tile_rows, tokens, first_expert, splits, tail_splits, sources),
        grid_spec=pltpu.PrefetchScalarGridSpec(
            num_scalar_prefetch=sources,
            grid=(experts, full_steps + 1),
            in_specs=[packed_spec] * sources + [in_spec, in_spec, down_spec],
            out_specs=[out_spec] * sources,
            scratch_shapes=[pltpu.VMEM((sources * rows, width), F32)],
        ),
        out_shape=[out] * sources,
        compiler_params=pltpu.CompilerParams(vmem_limit_bytes=VMEM_LIMIT),
        cost_estimate=pl.CostEstimate(flops=6 * sources * experts * rows * width * ff,
                                      bytes_accessed=6 * experts * width * ff, transcendentals=0),
        name="mlp",
    )(*metas, *packed, w_gate, w_up, w_down)


def mix_kernel(columns, starts_at, capacity, start_ref, base_ref, pos_ref, gate_ref, *rest):
    piece_refs, (out_ref, held_ref, sem) = rest[:-3], rest[-3:]
    step = pl.program_id(0)
    width = base_ref.shape[1]

    @pl.when(step == 0)
    def _():
        copies = []
        for n, piece in enumerate(piece_refs):
            first, at = starts_at[n]
            experts, rows = piece.shape[:2]
            copies.append(pltpu.make_async_copy(
                piece, held_ref.at[pl.ds(first, experts), pl.ds(at, rows), :], sem.at[n]))
        for copy in copies:
            copy.start()
        for copy in copies:
            copy.wait()

    def spans(window):
        for column in columns:
            begin = start_ref[column, step * (MIX_ROWS // LANES)]
            end = start_ref[column, (step + 1) * (MIX_ROWS // LANES)]
            base = pl.multiple_of(jnp.minimum((begin // 16) * 16, capacity - window), 16)
            yield base, end - base

    def mix(window):
        lane = lax.broadcasted_iota(I32, (MIX_ROWS, window), 1)
        bases = [base for base, _ in spans(window)]
        onehots = [(pos_ref[:, column:column + 1] - base == lane).astype(F32).astype(BF16)
                   for column, base in zip(columns, bases)]
        gates = [gate_ref[:, column:column + 1] for column in columns]
        for lo in range(0, width, MIX_COLS):
            cols = slice(lo, lo + MIX_COLS)
            total = base_ref[:, cols].astype(F32)
            for n in range(len(columns)):
                picked = jnp.dot(onehots[n], held_ref[n, pl.ds(bases[n], window), cols], preferred_element_type=F32)
                total = total + gates[n] * picked
            out_ref[:, cols] = total.astype(out_ref.dtype)

    fits = functools.reduce(jnp.logical_and, [rows <= MIX_WIN for _, rows in spans(MIX_WIN)])
    pl.when(fits)(lambda: mix(MIX_WIN))
    pl.when(jnp.logical_not(fits))(lambda: mix(WIDE_WIN))


def mix_call(columns, capacity, starts, base, pos, gates, placed, out_dtype):
    starts_at, pieces = zip(*placed)
    tokens, width = base.shape
    block = pl.BlockSpec((MIX_ROWS, width), lambda i, s: (i, 0))
    small = pl.BlockSpec((MIX_ROWS, pos.shape[1]), lambda i, s: (i, 0))
    return pl.pallas_call(
        functools.partial(mix_kernel, columns, starts_at, capacity),
        grid_spec=pltpu.PrefetchScalarGridSpec(
            num_scalar_prefetch=1,
            grid=(tokens // MIX_ROWS,),
            in_specs=[block, small, small] + [pl.BlockSpec(memory_space=pl.ANY)] * len(pieces),
            out_specs=block,
            scratch_shapes=[pltpu.VMEM((len(columns), capacity, width), BF16), pltpu.SemaphoreType.DMA((len(pieces),))],
        ),
        out_shape=jax.ShapeDtypeStruct((tokens, width), out_dtype),
        compiler_params=pltpu.CompilerParams(vmem_limit_bytes=VMEM_LIMIT),
        cost_estimate=pl.CostEstimate(flops=2 * tokens * MIX_WIN * width * len(columns),
                                      bytes_accessed=tokens * width * 10, transcendentals=0),
        name="mix",
    )(starts, base, pos, gates, *pieces)


def solution(mesh):
    group_size = mesh.shape["ep"]
    rows_spec = P(("dp", "ep"))

    def swap(array, distance):
        return lax.ppermute(array, "ep", [(i, i ^ distance) for i in range(group_size)])

    def device_step(hidden, ln_gamma, ln_beta, w_router, w_gate, w_up, w_down, choice, mask_first, mask_second):
        tokens, _ = hidden.shape
        local = w_gate.shape[0]
        experts = local * group_size
        capacity = (10 * tokens + 4 * experts - 1) // (4 * experts)

        choice_t = choice.T
        first = (local * lax.axis_index("ep")).astype(I32)[None]
        table, rel_t, *metas = route_call(first, choice_t, experts, local, capacity)
        metas = [metas[0]] + [swap(metas[m], m) for m in range(1, group_size)]

        halves = []
        for part in range(2):
            halves.append(norm_call(part, 2, hidden, ln_gamma, ln_beta))

        sources = [halves, [swap(u, 1) for u in halves],
                   [swap(u, 2) for u in halves]]
        sources.append([swap(u, 1) for u in sources[2]])

        def pack(m):
            return pack_call(metas[m], *sources[m], capacity)

        packed = {}

        def run(places, begin, rows, tile_rows, first_expert=0, count=local):
            return mlp_call(tokens, begin, rows, tile_rows, first_expert, count, [metas[m] for m in places],
                            [packed[m] for m in places], w_gate, w_up, w_down)

        late = capacity - LATE_ROWS
        final = late // FAR_TILE * FAR_TILE
        packed[0], packed[1] = pack(0), pack(1)
        near_early = run((0, 1), 0, late, NEAR_TILE)
        near_rows = [((0, 0), near_early[0]), ((local, 0), swap(near_early[1], 1))]

        packed[2], packed[3] = pack(2), pack(3)
        far_rows = []

        def send_far(expert, at, two, three):
            far_rows.append(((expert, at), swap(two, 2)))
            far_rows.append(((local + expert, at), swap(three, 3)))

        for c in range(final // FAR_TILE):
            send_far(0, c * FAR_TILE, *run((2, 3), c * FAR_TILE, FAR_TILE, FAR_TILE))
        zero, one, two, three = run((0, 1, 2, 3), late, LATE_ROWS, LATE_TILE)
        send_far(0, late, two, three)
        near_rows += [((0, late), zero), ((local, late), swap(one, 1))]
        for e in range(local):
            send_far(e, final, *run((2, 3), final, late - final, late - final, e, 1))

        gates = [gate_call(part, u, w_router.T, choice_t, rel_t, mask_first.T, mask_second.T)
                 for part, u in enumerate(halves)]
        gates_t = jnp.concatenate(gates, axis=1).T
        pos_t = table[:, :tokens].T
        marks = table[:, tokens:]
        total = mix_call(tuple(range(2 * local)), capacity, marks, hidden, pos_t, gates_t, near_rows, F32)
        return mix_call(tuple(range(2 * local, experts)), capacity, marks, total, pos_t, gates_t, far_rows, BF16)

    return jax.shard_map(device_step, mesh=mesh,
                         in_specs=(rows_spec, P(), P(), P(), P("ep"), P("ep"), P("ep"), rows_spec, rows_spec, rows_spec),
                         out_specs=rows_spec, check_vma=False)
```

```python
import functools

import jax
import jax.numpy as jnp
from jax import lax
from jax.experimental import pallas as pl
from jax.experimental.pallas import tpu as pltpu
from jax.sharding import PartitionSpec as P


LN_EPS = 1e-5
F32, BF16, I32 = jnp.float32, jnp.bfloat16, jnp.int32
VMEM_LIMIT = 67043328
NORM_ROWS = 256
GATE_ROWS = 512
PACK_ROWS = 256
PACK_WIN = 128
FAR_TILE = 192
NEAR_TILE = 256
LATE_TILE = 64
LATE_ROWS = 128
FF_BLOCK = 1280
FF_SPLIT = 768
MIX_ROWS = 512
MIX_WIN = 256
WIDE_WIN = 528
LANES = 128
MIX_COLS = 256


def route_kernel(capacity, first_ref, choice_ref, table_ref, rel_ref, *meta_refs):
    experts = table_ref.shape[0]
    tokens = choice_ref.shape[1]
    rows = meta_refs[0].shape[0]
    rel = choice_ref[...] ^ first_ref[0]
    rel_ref[...] = rel
    ids = lax.broadcasted_iota(I32, (experts, LANES), 0)
    lane = lax.broadcasted_iota(I32, (experts, LANES), 1)
    earlier = (lax.broadcasted_iota(I32, (LANES, LANES), 0) < lax.broadcasted_iota(I32, (LANES, LANES), 1))
    earlier = earlier.astype(F32).astype(BF16)
    carry = jnp.zeros((experts, 1), F32)
    marks = jnp.zeros((experts, LANES), F32)

    def store(block, lo):
        table_ref[:, lo:lo + LANES] = block
        for m, ref in enumerate(meta_refs):
            ref[:, lo:lo + LANES] = block[m * rows:(m + 1) * rows, :]

    for n in range(tokens // LANES):
        lo = n * LANES
        hit = ((rel[0:1, lo:lo + LANES] == ids) | (rel[1:2, lo:lo + LANES] == ids)).astype(F32)
        before = jnp.dot(hit.astype(BF16), earlier, preferred_element_type=F32) + carry
        kept = (hit > 0) & (before < capacity)
        store(jnp.where(kept, before, -1.0).astype(I32), lo)
        marks = jnp.where(lane == n, carry, marks)
        carry = carry + jnp.sum(hit, axis=1, keepdims=True)
    marks = jnp.where(lane == tokens // LANES, carry, marks)
    store(jnp.minimum(marks, float(capacity)).astype(I32), tokens)


def route_call(first, choice_t, experts, local, capacity):
    tokens = choice_t.shape[1]
    table = lambda n: jax.ShapeDtypeStruct((n, tokens + LANES), I32)
    return pl.pallas_call(
        functools.partial(route_kernel, capacity),
        in_specs=[pl.BlockSpec(memory_space=pltpu.SMEM), pl.BlockSpec(memory_space=pltpu.VMEM)],
        out_specs=[pl.BlockSpec(memory_space=pltpu.VMEM)] * (2 + experts // local),
        out_shape=[table(experts), jax.ShapeDtypeStruct((2, tokens), I32)] + [table(local)] * (experts // local),
        cost_estimate=pl.CostEstimate(flops=1 << 24, bytes_accessed=1 << 18, transcendentals=0),
        name="route",
    )(first, choice_t)


def norm_kernel(x_ref, gamma_ref, beta_ref, u_ref):
    values = x_ref[...].astype(F32)
    centred = values - jnp.mean(values, axis=-1, keepdims=True)
    variance = jnp.mean(centred * centred, axis=-1, keepdims=True)
    normed = centred * lax.rsqrt(variance + LN_EPS) * gamma_ref[...][None, :] + beta_ref[...][None, :]
    u_ref[...] = normed.astype(BF16)


def norm_call(part, parts, hidden, gamma, beta):
    tokens, width = hidden.shape
    rows = tokens // parts
    steps = rows // NORM_ROWS
    vector = pl.BlockSpec((width,), lambda i: (0,))
    return pl.pallas_call(
        norm_kernel,
        grid=(steps,),
        in_specs=[pl.BlockSpec((NORM_ROWS, width), lambda i: (i + part * steps, 0)), vector, vector],
        out_specs=pl.BlockSpec((NORM_ROWS, width), lambda i: (i, 0)),
        out_shape=jax.ShapeDtypeStruct((rows, width), BF16),
        compiler_params=pltpu.CompilerParams(vmem_limit_bytes=VMEM_LIMIT),
        cost_estimate=pl.CostEstimate(flops=rows * width * 60, bytes_accessed=rows * width * 4, transcendentals=0),
        name="norm",
    )(hidden, gamma, beta)


def gate_kernel(u_ref, router_ref, choice_ref, rel_ref, first_ref, second_ref, gate_ref):
    scores = lax.dot_general(router_ref[...], u_ref[...], (((1,), (1,)), ((), ())), preferred_element_type=F32)
    expert_ids = lax.broadcasted_iota(I32, scores.shape, 0)
    gates = jnp.zeros_like(scores)
    for j, mask_ref in enumerate((first_ref, second_ref)):
        masked = jnp.where(mask_ref[...] > 0, scores, -jnp.inf)
        weights = jnp.exp(masked - jnp.max(masked, axis=0, keepdims=True))
        picked = jnp.where(expert_ids == choice_ref[j:j + 1, :], weights, 0.0)
        gate = jnp.sum(picked, axis=0, keepdims=True) / jnp.sum(weights, axis=0, keepdims=True)
        gates = gates + jnp.where(expert_ids == rel_ref[j:j + 1, :], gate, 0.0)
    gate_ref[...] = gates


def gate_call(part, u, router_t, choice_t, rel_t, first_t, second_t):
    rows, width = u.shape
    experts = router_t.shape[0]
    steps = rows // GATE_ROWS
    lanes = lambda n: pl.BlockSpec((n, GATE_ROWS), lambda i: (0, i + part * steps))
    return pl.pallas_call(
        gate_kernel,
        grid=(steps,),
        in_specs=[pl.BlockSpec((GATE_ROWS, width), lambda i: (i, 0)), pl.BlockSpec((experts, width), lambda i: (0, 0)),
                  lanes(2), lanes(2), lanes(experts), lanes(experts)],
        out_specs=pl.BlockSpec((experts, GATE_ROWS), lambda i: (0, i)),
        out_shape=jax.ShapeDtypeStruct((experts, rows), F32),
        compiler_params=pltpu.CompilerParams(vmem_limit_bytes=VMEM_LIMIT),
        cost_estimate=pl.CostEstimate(flops=rows * width * 60, bytes_accessed=rows * width * 2, transcendentals=0),
        name="gate",
    )(u, router_t, choice_t, rel_t, first_t, second_t)


def mark(tokens, rows, block):
    return tokens + block * (rows // LANES)


def pack_kernel(half_steps, meta_ref, pos_ref, low_ref, high_ref, rows_ref, block_ref, sem):
    step = pl.program_id(0)
    experts = rows_ref.shape[0]
    tokens = 2 * half_steps * PACK_ROWS

    def fetch(half_ref, n, slot):
        return pltpu.make_async_copy(half_ref.at[pl.ds(n * PACK_ROWS, PACK_ROWS), :], block_ref.at[slot], sem.at[slot])

    @pl.when(step == 0)
    def _():
        for h, half_ref in enumerate((low_ref, high_ref)):
            for n in range(half_steps):
                fetch(half_ref, n, h * half_steps + n).start()
        rows_ref[...] = jnp.zeros_like(rows_ref)

    fetch(low_ref, 0, step).wait()
    taken_ref = block_ref.at[step]
    sublane = lax.broadcasted_iota(I32, (PACK_WIN, PACK_ROWS), 0)
    spans, slots = [], []
    for e in range(experts):
        begin = meta_ref[e, mark(tokens, PACK_ROWS, step)]
        base = (begin // 16) * 16
        spans.append((base, meta_ref[e, mark(tokens, PACK_ROWS, step + 1)] - base))
        slots.append(jnp.broadcast_to(pos_ref[e:e + 1, :], (PACK_WIN, PACK_ROWS)))

    def onehot(e, at):
        return (slots[e] - at == sublane).astype(F32)

    def put(e, at, picked):
        head, body = pl.ds(pl.multiple_of(at, 16), 16), pl.ds(pl.multiple_of(at + 16, 16), PACK_WIN - 16)
        rows_ref[e, head, :] = (rows_ref[e, head, :].astype(F32) + picked[:16]).astype(BF16)
        rows_ref[e, body, :] = picked[16:].astype(BF16)

    joined = jnp.concatenate([onehot(e, spans[e][0]) for e in range(experts)], axis=0).astype(BF16)
    picked = jnp.dot(joined, taken_ref[...], preferred_element_type=F32)
    for e in range(experts):
        put(e, spans[e][0], picked[e * PACK_WIN:(e + 1) * PACK_WIN])

        def window(w, carry):
            at = spans[e][0] + w * PACK_WIN
            put(e, at, jnp.dot(onehot(e, at).astype(BF16), taken_ref[...], preferred_element_type=F32))
            return carry

        lax.fori_loop(1, (spans[e][1] + PACK_WIN - 1) // PACK_WIN, window, 0)


def pack_call(meta, low, high, capacity):
    half, width = low.shape
    experts = meta.shape[0]
    half_steps = half // PACK_ROWS
    padded = (capacity + PACK_WIN - 1) // PACK_WIN * PACK_WIN + PACK_WIN
    return pl.pallas_call(
        functools.partial(pack_kernel, half_steps),
        grid_spec=pltpu.PrefetchScalarGridSpec(
            num_scalar_prefetch=1,
            grid=(2 * half_steps,),
            in_specs=[pl.BlockSpec((experts, PACK_ROWS), lambda i, s: (0, i)),
                      pl.BlockSpec(memory_space=pl.ANY), pl.BlockSpec(memory_space=pl.ANY)],
            out_specs=pl.BlockSpec((experts, padded, width), lambda i, s: (0, 0, 0)),
            scratch_shapes=[pltpu.VMEM((2 * half_steps, PACK_ROWS, width), BF16),
                            pltpu.SemaphoreType.DMA((2 * half_steps,))],
        ),
        out_shape=jax.ShapeDtypeStruct((experts, padded, width), BF16),
        compiler_params=pltpu.CompilerParams(vmem_limit_bytes=VMEM_LIMIT),
        cost_estimate=pl.CostEstimate(flops=experts * 2 * half * PACK_ROWS * width, bytes_accessed=4 * half * width * 3,
                                      transcendentals=0),
        name="pack",
    )(meta, meta, low, high)


def row_tiles(begin, rows, tile, tokens, expert, meta_refs):
    last = mark(tokens, tokens, 1)
    most = functools.reduce(jnp.maximum, [ref[expert, last] for ref in meta_refs])
    return jnp.clip((most - begin + tile - 1) // tile, 0, rows // tile)


def tail_step(turn, step, steps):
    return step == jnp.where(turn % 2 == 0, 0, steps - 1)


def mlp_kernel(begin, tile_rows, tokens, first_expert, splits, tail_splits, sources, *refs):
    meta_refs, row_refs = refs[:sources], refs[sources:2 * sources]
    gate_ref, up_ref, down_ref = refs[2 * sources:2 * sources + 3]
    out_refs, acc_ref = refs[2 * sources + 3:-1], refs[-1]
    turn, step, steps = pl.program_id(0), pl.program_id(1), pl.num_programs(1)
    rows = out_refs[0].shape[1]
    height = sources * tile_rows
    tiles = row_tiles(begin, rows, tile_rows, tokens, first_expert + turn, meta_refs)
    is_tail = tail_step(turn, step, steps)

    def accumulate(parts):
        def tile(i, carry):
            at = pl.multiple_of(i * tile_rows, tile_rows)
            held_rows = pl.ds(pl.multiple_of(i * height, height), height)
            taken = jnp.concatenate([ref[0, pl.ds(at, tile_rows), :] for ref in row_refs], axis=0)
            projs = []
            for lo, hi in parts:
                joined = jnp.concatenate([gate_ref[0, :, lo:hi], up_ref[0, :, lo:hi]], axis=1)
                projs.append(jnp.dot(taken, joined, preferred_element_type=F32))
            for n, (lo, hi) in enumerate(parts):
                inner = (jax.nn.silu(projs[n][:, :hi - lo]) * projs[n][:, hi - lo:]).astype(BF16)
                down = jnp.dot(inner, down_ref[0, lo:hi, :], preferred_element_type=F32)
                held = acc_ref[held_rows, :]
                if n == 0:
                    held = jnp.where(step == 0, 0.0, held)
                acc_ref[held_rows, :] = held + down
            return carry

        lax.fori_loop(0, tiles, tile, 0)

    pl.when(is_tail)(lambda: accumulate(tail_splits))
    pl.when(jnp.logical_not(is_tail))(lambda: accumulate(splits))

    @pl.when(step == steps - 1)
    def _():
        for i in range(rows // tile_rows):
            @pl.when(i < tiles)
            def _():
                for n, ref in enumerate(out_refs):
                    at = (sources * i + n) * tile_rows
                    ref[0, i * tile_rows:(i + 1) * tile_rows, :] = acc_ref[at:at + tile_rows, :].astype(BF16)

            @pl.when(i >= tiles)
            def _():
                for ref in out_refs:
                    ref[0, i * tile_rows:(i + 1) * tile_rows, :] = jnp.zeros((tile_rows, ref.shape[2]), BF16)


def mlp_call(tokens, begin, rows, tile_rows, first_expert, experts, metas, packed, w_gate, w_up, w_down):
    width, ff = w_gate.shape[1:]
    sources = len(metas)
    full_steps, tail = divmod(ff, FF_BLOCK)
    splits = ((0, FF_SPLIT), (FF_SPLIT, FF_BLOCK))
    tail_splits = ((0, tail),)
    once = pl.Buffered(1)

    def block(e, f, refs):
        idle = row_tiles(begin, rows, tile_rows, tokens, first_expert + e, refs) == 0
        return jnp.where(tail_step(e, f, full_steps + 1) | idle, full_steps, jnp.where(e % 2 == 0, f - 1, f))

    packed_spec = pl.BlockSpec((1, rows, width), lambda e, f, *m: (first_expert + e, begin // rows, 0), pipeline_mode=once)
    out_spec = pl.BlockSpec((1, rows, width), lambda e, f, *m: (e, 0, 0), pipeline_mode=once)
    in_spec = pl.BlockSpec((1, width, FF_BLOCK), lambda e, f, *m: (first_expert + e, 0, block(e, f, m)))
    down_spec = pl.BlockSpec((1, FF_BLOCK, width), lambda e, f, *m: (first_expert + e, block(e, f, m), 0))
    out = jax.ShapeDtypeStruct((experts, rows, width), BF16)
    return pl.pallas_call(
        functools.partial(mlp_kernel, begin, tile_rows, tokens, first_expert, splits, tail_splits, sources),
        grid_spec=pltpu.PrefetchScalarGridSpec(
            num_scalar_prefetch=sources,
            grid=(experts, full_steps + 1),
            in_specs=[packed_spec] * sources + [in_spec, in_spec, down_spec],
            out_specs=[out_spec] * sources,
            scratch_shapes=[pltpu.VMEM((sources * rows, width), F32)],
        ),
        out_shape=[out] * sources,
        compiler_params=pltpu.CompilerParams(vmem_limit_bytes=VMEM_LIMIT),
        cost_estimate=pl.CostEstimate(flops=6 * sources * experts * rows * width * ff,
                                      bytes_accessed=6 * experts * width * ff, transcendentals=0),
        name="mlp",
    )(*metas, *packed, w_gate, w_up, w_down)


def mix_kernel(columns, starts_at, capacity, start_ref, base_ref, pos_ref, gate_ref, *rest):
    piece_refs, (out_ref, held_ref, sem) = rest[:-3], rest[-3:]
    step = pl.program_id(0)
    width = base_ref.shape[1]

    @pl.when(step == 0)
    def _():
        copies = []
        for n, piece in enumerate(piece_refs):
            first, at = starts_at[n]
            experts, rows = piece.shape[:2]
            copies.append(pltpu.make_async_copy(
                piece, held_ref.at[pl.ds(first, experts), pl.ds(at, rows), :], sem.at[n]))
        for copy in copies:
            copy.start()
        for copy in copies:
            copy.wait()

    def spans(window):
        for column in columns:
            begin = start_ref[column, step * (MIX_ROWS // LANES)]
            end = start_ref[column, (step + 1) * (MIX_ROWS // LANES)]
            base = pl.multiple_of(jnp.minimum((begin // 16) * 16, capacity - window), 16)
            yield base, end - base

    def mix(window):
        lane = lax.broadcasted_iota(I32, (MIX_ROWS, window), 1)
        bases = [base for base, _ in spans(window)]
        onehots = [(pos_ref[:, column:column + 1] - base == lane).astype(F32).astype(BF16)
                   for column, base in zip(columns, bases)]
        gates = [gate_ref[:, column:column + 1] for column in columns]
        for lo in range(0, width, MIX_COLS):
            cols = slice(lo, lo + MIX_COLS)
            total = base_ref[:, cols].astype(F32)
            for n in range(len(columns)):
                picked = jnp.dot(onehots[n], held_ref[n, pl.ds(bases[n], window), cols], preferred_element_type=F32)
                total = total + gates[n] * picked
            out_ref[:, cols] = total.astype(out_ref.dtype)

    fits = functools.reduce(jnp.logical_and, [rows <= MIX_WIN for _, rows in spans(MIX_WIN)])
    pl.when(fits)(lambda: mix(MIX_WIN))
    pl.when(jnp.logical_not(fits))(lambda: mix(WIDE_WIN))


def mix_call(columns, capacity, starts, base, pos, gates, placed, out_dtype):
    starts_at, pieces = zip(*placed)
    tokens, width = base.shape
    block = pl.BlockSpec((MIX_ROWS, width), lambda i, s: (i, 0))
    small = pl.BlockSpec((MIX_ROWS, pos.shape[1]), lambda i, s: (i, 0))
    return pl.pallas_call(
        functools.partial(mix_kernel, columns, starts_at, capacity),
        grid_spec=pltpu.PrefetchScalarGridSpec(
            num_scalar_prefetch=1,
            grid=(tokens // MIX_ROWS,),
            in_specs=[block, small, small] + [pl.BlockSpec(memory_space=pl.ANY)] * len(pieces),
            out_specs=block,
            scratch_shapes=[pltpu.VMEM((len(columns), capacity, width), BF16), pltpu.SemaphoreType.DMA((len(pieces),))],
        ),
        out_shape=jax.ShapeDtypeStruct((tokens, width), out_dtype),
        compiler_params=pltpu.CompilerParams(vmem_limit_bytes=VMEM_LIMIT),
        cost_estimate=pl.CostEstimate(flops=2 * tokens * MIX_WIN * width * len(columns),
                                      bytes_accessed=tokens * width * 10, transcendentals=0),
        name="mix",
    )(starts, base, pos, gates, *pieces)


def solution(mesh):
    group_size = mesh.shape["ep"]
    rows_spec = P(("dp", "ep"))

    def swap(array, distance):
        return lax.ppermute(array, "ep", [(i, i ^ distance) for i in range(group_size)])

    def device_step(hidden, ln_gamma, ln_beta, w_router, w_gate, w_up, w_down, choice, mask_first, mask_second):
        tokens, _ = hidden.shape
        local = w_gate.shape[0]
        experts = local * group_size
        capacity = (10 * tokens + 4 * experts - 1) // (4 * experts)

        choice_t = choice.T
        first = (local * lax.axis_index("ep")).astype(I32)[None]
        table, rel_t, *metas = route_call(first, choice_t, experts, local, capacity)
        metas = [metas[0]] + [swap(metas[m], m) for m in range(1, group_size)]

        halves = []
        for part in range(2):
            halves.append(norm_call(part, 2, hidden, ln_gamma, ln_beta))

        sources = [halves, [swap(u, 1) for u in halves],
                   [swap(u, 2) for u in halves]]
        sources.append([swap(u, 1) for u in sources[2]])

        def pack(m):
            return pack_call(metas[m], *sources[m], capacity)

        packed = {}

        def run(places, begin, rows, tile_rows, first_expert=0, count=local):
            return mlp_call(tokens, begin, rows, tile_rows, first_expert, count, [metas[m] for m in places],
                            [packed[m] for m in places], w_gate, w_up, w_down)

        late = capacity - LATE_ROWS
        final = late // FAR_TILE * FAR_TILE
        packed[0], packed[1] = pack(0), pack(1)
        near_early = run((0, 1), 0, late, NEAR_TILE)
        near_rows = [((0, 0), near_early[0]), ((local, 0), swap(near_early[1], 1))]

        packed[2], packed[3] = pack(2), pack(3)
        far_rows = []

        def send_far(expert, at, two, three):
            far_rows.append(((expert, at), swap(two, 2)))
            far_rows.append(((local + expert, at), swap(three, 3)))

        for c in range(final // FAR_TILE):
            send_far(0, c * FAR_TILE, *run((2, 3), c * FAR_TILE, FAR_TILE, FAR_TILE))
        zero, one, two, three = run((0, 1, 2, 3), late, LATE_ROWS, LATE_TILE)
        send_far(0, late, two, three)
        near_rows += [((0, late), zero), ((local, late), swap(one, 1))]
        for e in range(local):
            send_far(e, final, *run((2, 3), final, late - final, late - final, e, 1))

        gates = [gate_call(part, u, w_router.T, choice_t, rel_t, mask_first.T, mask_second.T)
                 for part, u in enumerate(halves)]
        gates_t = jnp.concatenate(gates, axis=1).T
        pos_t = table[:, :tokens].T
        marks = table[:, tokens:]
        total = mix_call(tuple(range(2 * local)), capacity, marks, hidden, pos_t, gates_t, near_rows, F32)
        return mix_call(tuple(range(2 * local, experts)), capacity, marks, total, pos_t, gates_t, far_rows, BF16)

    return jax.shard_map(device_step, mesh=mesh,
                         in_specs=(rows_spec, P(), P(), P(), P("ep"), P("ep"), P("ep"), rows_spec, rows_spec, rows_spec),
                         out_specs=rows_spec, check_vma=False)
```
